32 devices in a mesh: dp: 8 (over z, core), tensor: 4 (over y, x).
Axes of the slice: x: 2, y: 2, z: 4, core: 2. Of those that a mesh axis runs over, the one named last changes fastest.
Arguments:
- block_input: bfloat16 [8192, 2048], P(('dp', 'tensor')), may hold values from -6 to 6
- attn_gain: float32 [2048], replicated, may hold values from 0.5 to 1.5
- w_query: bfloat16 [2048, 2048], P('dp', 'tensor'), may hold values from -6 to 6
- w_key: bfloat16 [2048, 512], P('dp', 'tensor'), may hold values from -0.125 to 0.125
- w_value: bfloat16 [2048, 512], P('dp', 'tensor'), may hold values from -0.125 to 0.125
- w_out: bfloat16 [2048, 2048], P('dp', 'tensor'), may hold values from -0.5 to 0.5
- mlp_gain: float32 [2048], replicated, may hold values from 0.5 to 1.5
- w_gate: bfloat16 [2048, 8192], P('dp', 'tensor'), may hold values from -0.125 to 0.125
- w_up: bfloat16 [2048, 8192], P('dp', 'tensor'), may hold values from -0.125 to 0.125
- w_down: bfloat16 [2048, 8192], P('dp', 'tensor'), may hold values from -0.0625 to 0.0625
- doc_ids: int32 [8192], P('dp'), may hold values from -1 to 3, as said below
- cotangent: bfloat16 [8192, 2048], P(('dp', 'tensor')), may hold values from -6 to 6
Outputs:
- block_output: bfloat16 [8192, 2048], P(('dp', 'tensor'))
- input_grad: bfloat16 [8192, 2048], P(('dp', 'tensor'))
- grad_query: float32 [2048, 2048], P('dp', 'tensor')
- grad_key: float32 [2048, 512], P('dp', 'tensor')
- grad_value: float32 [2048, 512], P('dp', 'tensor')
- grad_out: float32 [2048, 2048], P('dp', 'tensor')
- grad_gate: float32 [2048, 8192], P('dp', 'tensor')
- grad_up: float32 [2048, 8192], P('dp', 'tensor')
- grad_down: float32 [2048, 8192], P('dp', 'tensor')
- grad_attn_gain: float32 [2048], replicated
- grad_mlp_gain: float32 [2048], replicated
The draws below stay inside these ranges and needn't reach their ends.
Inputs may be any that keep to these rules, and one draw needn't show every extreme that they name: `doc_ids`: within each aligned block of 512 positions the ids of live positions never fall; -1 marks padding, which only ends a block; a block whose first position is -1 is padding throughout; every block ends with padding; a live block has at least 256 live positions; some index of dp has all its 2 blocks live, others may have fewer.
All inputs are finite; a program needn't handle non-finite values.
Results may differ from the reference program's by a relative error of at most 0.014.
The reference program's roundings to bfloat16 on the way count: a program that leaves them out, or rounds other values in their place, can miss the bound.
Values may be sent and summed in bfloat16 or wider, within the bound.
A program may use at most 256 MiB of HBM per device.

```python
import jax
import jax.numpy as jnp
from jax import lax

D = 2048
H = 32
KV = 8
HD = 64
FF = 8192
SEQ = 512
SLOTS = 2
TOK_DEV = 1024
TOKENS = 8192


def draw_w_query(key, part):
    keys_split = jax.random.split(key, 1)
    entries = jnp.clip(jax.random.normal(keys_split[0], (D, H * HD), jnp.float32), -4.0, 4.0) * D ** (-0.5)
    return jnp.clip(entries, -6.0, 6.0).astype(jnp.bfloat16)


def draw_doc_ids(key, part):
    group_total = TOKENS // TOK_DEV
    block_total = TOKENS // SEQ
    keys_split = jax.random.split(key, 4)
    live_count = jax.random.randint(keys_split[0], (group_total,), 1, SLOTS + 1)
    full_group = jax.random.randint(keys_split[1], (), 0, group_total)
    live_count = jnp.where(jnp.arange(group_total) == full_group, SLOTS, live_count)
    slot_index = jnp.arange(block_total) % SLOTS
    group_index = jnp.arange(block_total) // SLOTS
    live_block = slot_index < live_count[group_index]
    length = jax.random.randint(keys_split[2], (block_total,), SEQ // 2, SEQ)
    cut_points = jax.random.randint(keys_split[3], (block_total, 3), 1, SEQ // 2)
    positions = jnp.arange(SEQ)
    doc_index = jnp.sum((positions[None, :, None] >= cut_points[:, None, :]).astype(jnp.int32), axis=2)
    live_mask = live_block[:, None] & (positions[None, :] < length[:, None])
    return jnp.where(live_mask, doc_index, -1).reshape(TOKENS).astype(jnp.int32)


def with_spikes(array, rng, source, target, blocks, factor):
    def block_of(position):
        return (jnp.arange(array.shape[position]) // (array.shape[position] // blocks)).reshape((-1,) + (1,) * (array.ndim - 1 - position))

    first = jax.random.permutation(rng, blocks)[block_of(target)]
    far = (block_of(target) + blocks // 2) % blocks
    return jnp.where((block_of(source) == first) | (block_of(source) == far), factor * array, array)


def levels(rng, dims, cuts, least, largest):
    factor_of = 1.0
    for dim, parts in cuts:
        steps = jax.random.uniform(jax.random.fold_in(jax.random.fold_in(rng, 6), dim), (parts,), jnp.float32, least / len(cuts), largest / len(cuts))
        factor_of = factor_of * jnp.repeat(jnp.exp(steps), dims[dim] // parts).reshape((-1,) + (1,) * (len(dims) - 1 - dim))
    return factor_of


def bell_draw(rng, shape, spread, reach, shards=(), held_as=jnp.bfloat16):
    level = levels(rng, shape, shards, -0.22, 0.18) if shards else 1.0
    result = jax.random.normal(rng, shape, jnp.float32) * spread * level
    return jnp.minimum(jnp.maximum(result, -reach), reach).astype(held_as)


def gaussian_with(key, shape, scale, bound, cuts, heavy, kind=jnp.bfloat16):
    values = scale * jax.random.normal(key, shape, jnp.float32)
    if cuts:
        values = values * levels(key, shape, cuts, -0.22, 0.18)
    return jnp.clip(with_spikes(values, jax.random.fold_in(key, 3), *heavy), -bound, bound).astype(kind)


def setup_inputs(seed: int = 0) -> dict:
    seeds = jax.random.split(jax.random.key(seed), 13)
    block_input = bell_draw(seeds[0], (TOKENS, D), 1.0, 6.0, ((0, 32),))
    attn_gain = jnp.clip(1.0 + 0.1 * jax.random.normal(seeds[1], (D,), jnp.float32), 0.5, 1.5)
    w_query = draw_w_query(jax.random.fold_in(seeds[12], 71), 0)
    w_key = bell_draw(seeds[3], (D, KV * HD), D ** -0.5, 0.125, ((0, 8), (1, 4)))
    w_value = bell_draw(seeds[4], (D, KV * HD), D ** -0.5, 0.125, ((0, 8), (1, 4)))
    w_out = bell_draw(seeds[5], (D, H * HD), (H * HD // 16) ** -0.5, 0.5, ((0, 8), (1, 4)))
    mlp_gain = jnp.clip(1.0 + 0.1 * jax.random.normal(seeds[6], (D,), jnp.float32), 0.5, 1.5)
    w_gate = bell_draw(seeds[7], (D, FF), D ** -0.5, 0.125, ((0, 8), (1, 4)))
    w_up = bell_draw(seeds[8], (D, FF), D ** -0.5, 0.125, ((0, 8), (1, 4)))
    w_down = bell_draw(seeds[9], (D, FF), FF ** -0.5, 0.0625, ((0, 8), (1, 4)))
    doc_ids = draw_doc_ids(jax.random.fold_in(seeds[12], 71), 0)
    cotangent = gaussian_with(seeds[11], (TOKENS, D), 1.0, 6.0, ((0, 32),), (0, 1, 32, 2.75))
    return dict(block_input=block_input, attn_gain=attn_gain, w_query=w_query, w_key=w_key, w_value=w_value, w_out=w_out, mlp_gain=mlp_gain, w_gate=w_gate, w_up=w_up, w_down=w_down, doc_ids=doc_ids, cotangent=cotangent)


EPSILON = 1e-05
ROPE_BASE = 500000.0
NEG_LARGE = -1e+30

def round_bf(tensor_rows):
    return lax.optimization_barrier(tensor_rows.astype(jnp.bfloat16))

def rotary_tables(length, head_dim):
    half_dim = head_dim // 2
    frequency = ROPE_BASE ** (-(jnp.arange(half_dim, dtype=jnp.float32) * (2.0 / head_dim)))
    angles = jnp.arange(length, dtype=jnp.float32)[:, None] * frequency[None, :]
    angles = jnp.concatenate([angles, angles], axis=1)
    return (jnp.cos(angles), jnp.sin(angles))

def rotate_half(tensor_rows):
    half_dim = tensor_rows.shape[-1] // 2
    return jnp.concatenate([-tensor_rows[..., half_dim:], tensor_rows[..., :half_dim]], axis=-1)

def rotate_back(tensor_rows):
    half_dim = tensor_rows.shape[-1] // 2
    return jnp.concatenate([tensor_rows[..., half_dim:], -tensor_rows[..., :half_dim]], axis=-1)

def apply_rotary(tensor_rows, cosine_table, sine_table):
    return tensor_rows * cosine_table[:, None, :] + rotate_half(tensor_rows) * sine_table[:, None, :]

def undo_rotary(tensor_rows, cosine_table, sine_table):
    return tensor_rows * cosine_table[:, None, :] + rotate_back(tensor_rows * sine_table[:, None, :])

def norm_scale(tensor_rows):
    return lax.rsqrt(lax.optimization_barrier(jnp.mean(tensor_rows * tensor_rows, axis=1, keepdims=True)) + EPSILON)

def norm_back(grad_normed, tensor_rows, row_scale, gain_row):
    weighted = grad_normed * gain_row[None, :]
    inner_mean = lax.optimization_barrier(jnp.mean(weighted * tensor_rows, axis=1, keepdims=True))
    return row_scale * weighted - tensor_rows * (row_scale * row_scale * row_scale) * inner_mean

def slot_mask(doc_rows):
    positions = jnp.arange(doc_rows.shape[0])
    earlier = positions[None, :] <= positions[:, None]
    same_doc = (doc_rows[:, None] == doc_rows[None, :]) & (doc_rows[:, None] >= 0)
    return same_doc & earlier | (positions[None, :] == positions[:, None])

def contract_rows(left_side, right_side):
    return lax.dot_general(left_side, right_side, (((0,), (0,)), ((), ())), preferred_element_type=jnp.float32)

def contract_cols(left_side, right_side):
    return lax.dot_general(left_side, right_side, (((1,), (1,)), ((), ())), preferred_element_type=jnp.float32)

def slot_scores(query_rows, key_rows, allowed):
    seq_len, head_count, head_dim = query_rows.shape
    groups = key_rows.shape[1]
    grouped = query_rows.astype(jnp.float32).reshape(seq_len, groups, head_count // groups, head_dim)
    scores = jnp.einsum('sgjd,tgd->gjst', grouped, key_rows.astype(jnp.float32)) * head_dim ** (-0.5)
    return (grouped, jnp.where(allowed[None, None], scores, NEG_LARGE))

def attend(query_rows, key_rows, value_rows, allowed, live_rows):
    seq_len, head_count, head_dim = query_rows.shape
    grouped, scores = slot_scores(query_rows, key_rows, allowed)
    row_max = lax.optimization_barrier(jnp.max(scores, axis=-1, keepdims=True))
    weights = jnp.exp(scores - row_max)
    row_total = lax.optimization_barrier(jnp.sum(weights, axis=-1, keepdims=True))
    prob_bf = round_bf(weights / row_total).astype(jnp.float32)
    mixed_rows = jnp.einsum('gjst,tgd->sgjd', prob_bf, value_rows.astype(jnp.float32))
    mixed_rows = mixed_rows.reshape(seq_len, head_count * head_dim) * live_rows[:, None]
    return (round_bf(mixed_rows), row_max + jnp.log(row_total))

def attend_back(query_rows, key_rows, value_rows, allowed, log_total, grad_mixed):
    seq_len, head_count, head_dim = query_rows.shape
    groups = key_rows.shape[1]
    grouped, scores = slot_scores(query_rows, key_rows, allowed)
    prob_full = jnp.where(allowed[None, None], jnp.exp(scores - log_total), 0.0)
    grad_rows = grad_mixed.astype(jnp.float32).reshape(seq_len, groups, head_count // groups, head_dim)
    grad_prob = jnp.einsum('sgjd,tgd->gjst', grad_rows, value_rows.astype(jnp.float32))
    row_delta = lax.optimization_barrier(jnp.sum(prob_full * grad_prob, axis=-1, keepdims=True))
    grad_scores = round_bf(prob_full * (grad_prob - row_delta)).astype(jnp.float32)
    prob_bf = round_bf(prob_full).astype(jnp.float32)
    grad_values = jnp.einsum('gjst,sgjd->tgd', prob_bf, grad_rows)
    grad_queries = jnp.einsum('gjst,tgd->sgjd', grad_scores, key_rows.astype(jnp.float32)) * head_dim ** (-0.5)
    grad_keys = jnp.einsum('gjst,sgjd->tgd', grad_scores, grouped) * head_dim ** (-0.5)
    return (grad_queries.reshape(seq_len, head_count, head_dim), grad_keys, grad_values)

def reference(block_input, attn_gain, w_query, w_key, w_value, w_out, mlp_gain, w_gate, w_up, w_down, doc_ids, cotangent):
    cosine_table, sine_table = rotary_tables(SEQ, HD)
    slot_total = TOKENS // SEQ

    def one_slot(totals, packed):
        rows_in, doc_rows, grad_out_rows = packed
        input_f = rows_in.astype(jnp.float32)
        scale_one = norm_scale(input_f)
        normed_one = round_bf(input_f * scale_one * attn_gain[None, :])
        query_rows = round_bf(apply_rotary(jnp.dot(normed_one, w_query, preferred_element_type=jnp.float32).reshape(SEQ, H, HD), cosine_table, sine_table))
        key_rows = round_bf(apply_rotary(jnp.dot(normed_one, w_key, preferred_element_type=jnp.float32).reshape(SEQ, KV, HD), cosine_table, sine_table))
        value_rows = round_bf(jnp.dot(normed_one, w_value, preferred_element_type=jnp.float32)).reshape(SEQ, KV, HD)
        allowed = slot_mask(doc_rows)
        live_rows = (doc_rows >= 0).astype(jnp.float32)
        mixed_rows, log_total = attend(query_rows, key_rows, value_rows, allowed, live_rows)
        residual = input_f + contract_cols(mixed_rows, w_out)
        scale_two = norm_scale(residual)
        normed_two = round_bf(residual * scale_two * mlp_gain[None, :])
        gate_pre = jnp.dot(normed_two, w_gate, preferred_element_type=jnp.float32)
        up_pre = jnp.dot(normed_two, w_up, preferred_element_type=jnp.float32)
        sigmoid_gate = jax.nn.sigmoid(gate_pre)
        silu_gate = gate_pre * sigmoid_gate
        hidden = round_bf(silu_gate * up_pre)
        out_rows = (residual + contract_cols(hidden, w_down)).astype(jnp.bfloat16)
        grad_hidden = jnp.dot(grad_out_rows, w_down, preferred_element_type=jnp.float32)
        grad_down = contract_rows(grad_out_rows, hidden)
        grad_gate_pre = round_bf(grad_hidden * up_pre * sigmoid_gate * (1.0 + gate_pre * (1.0 - sigmoid_gate)))
        grad_up_pre = round_bf(grad_hidden * silu_gate)
        grad_gate = contract_rows(normed_two, grad_gate_pre)
        grad_up = contract_rows(normed_two, grad_up_pre)
        grad_normed_two = contract_cols(grad_gate_pre, w_gate) + contract_cols(grad_up_pre, w_up)
        grad_mlp_gain = lax.optimization_barrier(jnp.sum(grad_normed_two * residual * scale_two, axis=0))
        grad_residual = grad_out_rows.astype(jnp.float32) + norm_back(grad_normed_two, residual, scale_two, mlp_gain)
        grad_residual_bf = round_bf(grad_residual)
        grad_out = contract_rows(grad_residual_bf, mixed_rows)
        grad_mixed = round_bf(jnp.dot(grad_residual_bf, w_out, preferred_element_type=jnp.float32) * live_rows[:, None])
        grad_queries, grad_keys, grad_values = attend_back(query_rows, key_rows, value_rows, allowed, log_total, grad_mixed)
        grad_query_rows = round_bf(undo_rotary(grad_queries, cosine_table, sine_table)).reshape(SEQ, H * HD)
        grad_key_rows = round_bf(undo_rotary(grad_keys, cosine_table, sine_table)).reshape(SEQ, KV * HD)
        grad_value_rows = round_bf(grad_values).reshape(SEQ, KV * HD)
        grad_query = contract_rows(normed_one, grad_query_rows)
        grad_key = contract_rows(normed_one, grad_key_rows)
        grad_value = contract_rows(normed_one, grad_value_rows)
        grad_normed_one = contract_cols(grad_query_rows, w_query) + contract_cols(grad_key_rows, w_key) + contract_cols(grad_value_rows, w_value)
        grad_attn_gain = lax.optimization_barrier(jnp.sum(grad_normed_one * input_f * scale_one, axis=0))
        grad_in = (grad_residual + norm_back(grad_normed_one, input_f, scale_one, attn_gain)).astype(jnp.bfloat16)
        terms = (grad_query, grad_key, grad_value, grad_out, grad_gate, grad_up, grad_down, grad_attn_gain, grad_mlp_gain)
        totals = tuple((running + term for running, term in zip(totals, terms)))
        return (totals, (out_rows, grad_in))
    start_totals = (jnp.zeros((D, H * HD), jnp.float32), jnp.zeros((D, KV * HD), jnp.float32), jnp.zeros((D, KV * HD), jnp.float32), jnp.zeros((D, H * HD), jnp.float32), jnp.zeros((D, FF), jnp.float32), jnp.zeros((D, FF), jnp.float32), jnp.zeros((D, FF), jnp.float32), jnp.zeros((D,), jnp.float32), jnp.zeros((D,), jnp.float32))
    packed_all = (block_input.reshape(slot_total, SEQ, D), doc_ids.reshape(slot_total, SEQ), cotangent.reshape(slot_total, SEQ, D))
    totals, (outputs, grads_in) = lax.scan(one_slot, start_totals, packed_all)
    return (outputs.reshape(TOKENS, D), grads_in.reshape(TOKENS, D), totals[0], totals[1], totals[2], totals[3], totals[4], totals[5], totals[6], totals[7], totals[8])
```

```python
import jax
import jax.numpy as jnp
from jax import lax
from jax.sharding import PartitionSpec as P

HD = 64
SEQ = 512


EPSILON = 1e-05
ROPE_BASE = 500000.0
NEG_LARGE = -1e30


def rotary_tables(length, head_dim):
    half_dim = head_dim // 2
    frequency = ROPE_BASE ** (-(jnp.arange(half_dim, dtype=jnp.float32) * (2.0 / head_dim)))
    angles = jnp.arange(length, dtype=jnp.float32)[:, None] * frequency[None, :]
    angles = jnp.concatenate([angles, angles], axis=1)
    return (jnp.cos(angles), jnp.sin(angles))


def rotate_half(tensor_rows):
    half_dim = tensor_rows.shape[-1] // 2
    return jnp.concatenate([-tensor_rows[..., half_dim:], tensor_rows[..., :half_dim]], axis=-1)


def rotate_back(tensor_rows):
    half_dim = tensor_rows.shape[-1] // 2
    return jnp.concatenate([tensor_rows[..., half_dim:], -tensor_rows[..., :half_dim]], axis=-1)


def apply_rotary(tensor_rows, cosine_table, sine_table):
    return (
        tensor_rows * cosine_table[:, None, :] + rotate_half(tensor_rows) * sine_table[:, None, :]
    )


def undo_rotary(tensor_rows, cosine_table, sine_table):
    return tensor_rows * cosine_table[:, None, :] + rotate_back(
        tensor_rows * sine_table[:, None, :]
    )


def norm_scale(tensor_rows):
    return lax.rsqrt(jnp.mean(tensor_rows * tensor_rows, axis=1, keepdims=True) + EPSILON)


def norm_back(grad_normed, tensor_rows, row_scale, gain_row):
    weighted = grad_normed * gain_row[None, :]
    inner_mean = jnp.mean(weighted * tensor_rows, axis=1, keepdims=True)
    return row_scale * weighted - tensor_rows * (row_scale * row_scale * row_scale) * inner_mean


def slot_mask(doc_rows):
    positions = jnp.arange(doc_rows.shape[0])
    earlier = positions[None, :] <= positions[:, None]
    same_doc = (doc_rows[:, None] == doc_rows[None, :]) & (doc_rows[:, None] >= 0)
    return same_doc & earlier | (positions[None, :] == positions[:, None])


def contract_rows(left_side, right_side):
    return lax.dot_general(
        left_side, right_side, (((0,), (0,)), ((), ())), preferred_element_type=jnp.float32
    )


def contract_cols(left_side, right_side):
    return lax.dot_general(
        left_side, right_side, (((1,), (1,)), ((), ())), preferred_element_type=jnp.float32
    )


def slot_scores(query_rows, key_rows, allowed):
    seq_len, head_count, head_dim = query_rows.shape
    groups = key_rows.shape[1]
    grouped = query_rows.reshape(seq_len, groups, head_count // groups, head_dim)
    scores = jnp.einsum(
        "sgjd,tgd->gjst", grouped, key_rows, preferred_element_type=jnp.float32
    ) * head_dim ** (-0.5)
    return (grouped, jnp.where(allowed[None, None], scores, NEG_LARGE))


def attend(packed):
    query_rows, key_rows, value_rows, doc_rows = packed
    seq_len, head_count, head_dim = query_rows.shape
    allowed = slot_mask(doc_rows)
    live_rows = (doc_rows >= 0).astype(jnp.float32)
    grouped, scores = slot_scores(query_rows, key_rows, allowed)
    row_max = jnp.max(scores, axis=-1, keepdims=True)
    weights = jnp.exp(scores - row_max)
    row_total = jnp.sum(weights, axis=-1, keepdims=True)
    prob_bf = (weights / row_total).astype(jnp.bfloat16)
    mixed_rows = jnp.einsum(
        "gjst,tgd->sgjd", prob_bf, value_rows, preferred_element_type=jnp.float32
    )
    mixed_rows = mixed_rows.reshape(seq_len, head_count * head_dim) * live_rows[:, None]
    return (mixed_rows.astype(jnp.bfloat16), row_max + jnp.log(row_total))


def attend_back(packed):
    query_rows, key_rows, value_rows, doc_rows, log_total, grad_mixed = packed
    seq_len, head_count, head_dim = query_rows.shape
    groups = key_rows.shape[1]
    allowed = slot_mask(doc_rows)
    grouped, scores = slot_scores(query_rows, key_rows, allowed)
    prob_full = jnp.where(allowed[None, None], jnp.exp(scores - log_total), 0.0)
    grad_rows = grad_mixed.reshape(seq_len, groups, head_count // groups, head_dim)
    grad_prob = jnp.einsum(
        "sgjd,tgd->gjst", grad_rows, value_rows, preferred_element_type=jnp.float32
    )
    row_delta = jnp.sum(prob_full * grad_prob, axis=-1, keepdims=True)
    grad_scores = (prob_full * (grad_prob - row_delta)).astype(jnp.bfloat16)
    grad_values = jnp.einsum(
        "gjst,sgjd->tgd",
        prob_full.astype(jnp.bfloat16),
        grad_rows,
        preferred_element_type=jnp.float32,
    )
    grad_queries = jnp.einsum(
        "gjst,tgd->sgjd", grad_scores, key_rows, preferred_element_type=jnp.float32
    ) * head_dim ** (-0.5)
    grad_keys = jnp.einsum(
        "gjst,sgjd->tgd", grad_scores, grouped, preferred_element_type=jnp.float32
    ) * head_dim ** (-0.5)
    return (grad_queries.reshape(seq_len, head_count, head_dim), grad_keys, grad_values)


def sum_rows(partial, axis):
    return lax.psum_scatter(
        partial.astype(jnp.bfloat16), axis, scatter_dimension=0, tiled=True
    ).astype(jnp.float32)


def per_device(
    block_input,
    attn_gain,
    w_query,
    w_key,
    w_value,
    w_out,
    mlp_gain,
    w_gate,
    w_up,
    w_down,
    doc_ids,
    cotangent,
):
    query_full, key_full, value_full, out_full, gate_full, up_full, down_full = (
        lax.all_gather(w_query, "dp", axis=0, tiled=True),
        lax.all_gather(w_key, "dp", axis=0, tiled=True),
        lax.all_gather(w_value, "dp", axis=0, tiled=True),
        lax.all_gather(w_out, "dp", axis=0, tiled=True),
        lax.all_gather(w_gate, "dp", axis=0, tiled=True),
        lax.all_gather(w_up, "dp", axis=0, tiled=True),
        lax.all_gather(w_down, "dp", axis=0, tiled=True),
    )
    total_rows = doc_ids.shape[0]
    slot_count = total_rows // SEQ
    local_heads = query_full.shape[1] // HD
    local_groups = key_full.shape[1] // HD
    cosine_table, sine_table = rotary_tables(SEQ, HD)
    live_all = (doc_ids >= 0).astype(jnp.float32)
    input_own = block_input.astype(jnp.float32)
    scale_one = norm_scale(input_own)
    normed_one = lax.all_gather(
        (input_own * scale_one * attn_gain[None, :]).astype(jnp.bfloat16),
        "tensor",
        axis=0,
        tiled=True,
    )
    query_pre = jnp.dot(normed_one, query_full, preferred_element_type=jnp.float32).reshape(
        slot_count, SEQ, local_heads, HD
    )
    key_pre = jnp.dot(normed_one, key_full, preferred_element_type=jnp.float32).reshape(
        slot_count, SEQ, local_groups, HD
    )
    query_rows = apply_rotary(query_pre, cosine_table, sine_table).astype(jnp.bfloat16)
    key_rows = apply_rotary(key_pre, cosine_table, sine_table).astype(jnp.bfloat16)
    value_rows = (
        jnp.dot(normed_one, value_full, preferred_element_type=jnp.float32)
        .astype(jnp.bfloat16)
        .reshape(slot_count, SEQ, local_groups, HD)
    )
    doc_slots = doc_ids.reshape(slot_count, SEQ)
    mixed_slots, log_total = lax.map(attend, (query_rows, key_rows, value_rows, doc_slots))
    mixed_all = mixed_slots.reshape(total_rows, local_heads * HD)
    residual_own = input_own + sum_rows(contract_cols(mixed_all, out_full), "tensor")
    scale_two_own = norm_scale(residual_own)
    normed_two = lax.all_gather(
        (residual_own * scale_two_own * mlp_gain[None, :]).astype(jnp.bfloat16),
        "tensor",
        axis=0,
        tiled=True,
    )
    gate_pre = jnp.dot(normed_two, gate_full, preferred_element_type=jnp.float32)
    up_pre = jnp.dot(normed_two, up_full, preferred_element_type=jnp.float32)
    sigmoid_gate = jax.nn.sigmoid(gate_pre)
    silu_gate = gate_pre * sigmoid_gate
    hidden = (silu_gate * up_pre).astype(jnp.bfloat16)
    block_output = (
        residual_own
        + sum_rows(contract_cols(hidden, down_full), "tensor")
    ).astype(jnp.bfloat16)
    grad_full = lax.all_gather(cotangent, "tensor", axis=0, tiled=True)
    grad_hidden = jnp.dot(grad_full, down_full, preferred_element_type=jnp.float32)
    grad_down = contract_rows(grad_full, hidden)
    grad_gate_pre = (
        grad_hidden * up_pre * sigmoid_gate * (1.0 + gate_pre * (1.0 - sigmoid_gate))
    ).astype(jnp.bfloat16)
    grad_up_pre = (grad_hidden * silu_gate).astype(jnp.bfloat16)
    grad_gate = contract_rows(normed_two, grad_gate_pre)
    grad_up = contract_rows(normed_two, grad_up_pre)
    grad_normed_own = sum_rows(
        contract_cols(grad_gate_pre, gate_full) + contract_cols(grad_up_pre, up_full),
        "tensor",
    )
    grad_mlp_gain = jnp.sum(grad_normed_own * residual_own * scale_two_own, axis=0)
    grad_residual_own = cotangent.astype(jnp.float32) + norm_back(
        grad_normed_own, residual_own, scale_two_own, mlp_gain
    )
    grad_residual_bf = lax.all_gather(
        grad_residual_own.astype(jnp.bfloat16), "tensor", axis=0, tiled=True
    )
    grad_out = contract_rows(grad_residual_bf, mixed_all)
    grad_mixed = (
        jnp.dot(grad_residual_bf, out_full, preferred_element_type=jnp.float32) * live_all[:, None]
    ).astype(jnp.bfloat16)
    grad_mixed_slots = grad_mixed.reshape(slot_count, SEQ, local_heads * HD)
    grad_queries, grad_keys, grad_values = lax.map(
        attend_back, (query_rows, key_rows, value_rows, doc_slots, log_total, grad_mixed_slots)
    )
    grad_query_rows = (
        undo_rotary(grad_queries, cosine_table, sine_table)
        .astype(jnp.bfloat16)
        .reshape(total_rows, local_heads * HD)
    )
    grad_key_rows = (
        undo_rotary(grad_keys, cosine_table, sine_table)
        .astype(jnp.bfloat16)
        .reshape(total_rows, local_groups * HD)
    )
    grad_value_rows = grad_values.astype(jnp.bfloat16).reshape(total_rows, local_groups * HD)
    grad_query = contract_rows(normed_one, grad_query_rows)
    grad_key = contract_rows(normed_one, grad_key_rows)
    grad_value = contract_rows(normed_one, grad_value_rows)
    grad_normed_one = sum_rows(
        contract_cols(grad_query_rows, query_full)
        + contract_cols(grad_key_rows, key_full)
        + contract_cols(grad_value_rows, value_full),
        "tensor",
    )
    grad_attn_gain = jnp.sum(grad_normed_one * input_own * scale_one, axis=0)
    input_grad = (
        grad_residual_own + norm_back(grad_normed_one, input_own, scale_one, attn_gain)
    ).astype(jnp.bfloat16)
    summed = (
        sum_rows(grad_query, "dp"),
        sum_rows(grad_key, "dp"),
        sum_rows(grad_value, "dp"),
        sum_rows(grad_out, "dp"),
        sum_rows(grad_gate, "dp"),
        sum_rows(grad_up, "dp"),
        sum_rows(grad_down, "dp"),
    )
    gains = lax.psum((grad_attn_gain, grad_mlp_gain), ("dp", "tensor"))
    return (
        block_output,
        input_grad,
        summed[0],
        summed[1],
        summed[2],
        summed[3],
        summed[4],
        summed[5],
        summed[6],
        gains[0],
        gains[1],
    )


def solution(mesh):
    in_specs = (
        P(("dp", "tensor"), None),
        P(),
        P("dp", "tensor"),
        P("dp", "tensor"),
        P("dp", "tensor"),
        P("dp", "tensor"),
        P(),
        P("dp", "tensor"),
        P("dp", "tensor"),
        P("dp", "tensor"),
        P("dp"),
        P(("dp", "tensor"), None),
    )
    out_specs = (
        P(("dp", "tensor"), None),
        P(("dp", "tensor"), None),
        P("dp", "tensor"),
        P("dp", "tensor"),
        P("dp", "tensor"),
        P("dp", "tensor"),
        P("dp", "tensor"),
        P("dp", "tensor"),
        P("dp", "tensor"),
        P(),
        P(),
    )
    return jax.shard_map(
        per_device, mesh=mesh, in_specs=in_specs, out_specs=out_specs, check_vma=False
    )
```

```python
import functools

import jax
import jax.numpy as jnp
from jax import lax
from jax.experimental import pallas as pl
from jax.experimental.pallas import tpu as pltpu
from jax.sharding import PartitionSpec as P

HD = 64
SEQ = 512
QUERY_TILE = 256

EPSILON = 1e-05
ROPE_BASE = 500000.0
NEG_LARGE = -1e30


def rotary_tables(length, head_dim, copies):
    half_dim = head_dim // 2
    frequency = ROPE_BASE ** (-(jnp.arange(half_dim, dtype=jnp.float32) * (2.0 / head_dim)))
    angles = jnp.arange(length, dtype=jnp.float32)[:, None] * frequency[None, :]
    angles = jnp.concatenate([angles, angles] * copies, axis=1)
    return (jnp.cos(angles), jnp.sin(angles))


def norm_scale(tensor_rows):
    return lax.rsqrt(jnp.mean(tensor_rows * tensor_rows, axis=1, keepdims=True) + EPSILON)


def norm_back(grad_normed, tensor_rows, row_scale, gain_row):
    weighted = grad_normed * gain_row[None, :]
    inner_mean = jnp.mean(weighted * tensor_rows, axis=1, keepdims=True)
    return row_scale * weighted - tensor_rows * (row_scale * row_scale * row_scale) * inner_mean


def contract_rows(left_side, right_side):
    return lax.dot_general(
        left_side, right_side, (((0,), (0,)), ((), ())), preferred_element_type=jnp.float32
    )


def contract_cols(left_side, right_side):
    return lax.dot_general(
        left_side, right_side, (((1,), (1,)), ((), ())), preferred_element_type=jnp.float32
    )


def matmul(left_side, right_side):
    return jnp.dot(left_side, right_side, preferred_element_type=jnp.float32)


def half_turn(rows):
    width = rows.shape[1]
    first = lax.broadcasted_iota(jnp.int32, rows.shape, 1) % HD < HD // 2
    if width % 128 == 0:
        later = pltpu.roll(rows, width - HD // 2, axis=1)
        before = pltpu.roll(rows, HD // 2, axis=1)
        return jnp.where(first, later, before), first
    halves = [rows[:, at : at + HD // 2] for at in range(0, width, HD // 2)]
    swapped = [halves[i ^ 1] for i in range(len(halves))]
    return jnp.concatenate(swapped, axis=1), first


def rotate(rows, cosine, sine):
    turned, first = half_turn(rows)
    return rows * cosine + jnp.where(first, -turned, turned) * sine


def unrotate(rows, cosine, sine):
    turned, first = half_turn(rows * sine)
    return rows * cosine + jnp.where(first, turned, -turned)


def group_columns(rows, group, groups):
    picked = rows[:, :HD]
    for other in range(1, groups):
        picked = jnp.where(group == other, rows[:, other * HD : (other + 1) * HD], picked)
    return picked


def tile_bias(doc_row, doc_col, start, tile, keys):
    query_doc = doc_row[0, :, start : start + tile]
    key_doc = doc_col[:keys, :]
    key_at = lax.broadcasted_iota(jnp.int32, (keys, tile), 0)
    query_at = lax.broadcasted_iota(jnp.int32, (keys, tile), 1) + start
    same = (query_doc == key_doc) & (key_doc >= 0) & (key_at <= query_at)
    live = (query_doc >= 0).astype(jnp.float32)
    return jnp.where(same | (key_at == query_at), 0.0, NEG_LARGE), live


def tile_probs(keys_rows, query_tile, bias):
    scores = contract_cols(keys_rows, query_tile) * HD ** (-0.5) + bias
    weights = jnp.exp(scores - jnp.max(scores, axis=0, keepdims=True))
    return weights * (1.0 / jnp.sum(weights, axis=0, keepdims=True))


def attend_kernel(
    groups, q_ref, k_ref, v_ref, row_ref, col_ref, cos_ref, sin_ref,
    q_out, k_out, v_out, mixed_ref
):
    group = pl.program_id(1)
    width = q_ref.shape[1]
    narrow = k_ref.shape[1]
    query_rows = rotate(q_ref[...], cos_ref[...], sin_ref[...]).astype(jnp.bfloat16)
    key_all = rotate(k_ref[...], cos_ref[:, :narrow], sin_ref[:, :narrow]).astype(jnp.bfloat16)
    value_all = v_ref[...].astype(jnp.bfloat16)
    q_out[...] = query_rows
    k_out[...] = key_all
    v_out[...] = value_all
    key_rows = group_columns(key_all, group, groups)
    value_rows = group_columns(value_all, group, groups)
    for start in range(0, SEQ, QUERY_TILE):
        keys = start + QUERY_TILE
        bias, live = tile_bias(row_ref, col_ref, start, QUERY_TILE, keys)
        mixed = []
        for head in range(width // HD):
            query_tile = query_rows[start:keys, head * HD : (head + 1) * HD]
            probs = tile_probs(key_rows[:keys], query_tile, bias).astype(jnp.bfloat16)
            mixed.append(contract_rows(value_rows[:keys], probs) * live)
        mixed_ref[start:keys, :] = jnp.concatenate(mixed, axis=0).T.astype(jnp.bfloat16)


def attend_back_kernel(
    groups, q_ref, k_ref, v_ref, grad_ref, row_ref, col_ref, cos_ref, sin_ref,
    dq_ref, dk_ref, dv_ref, dk_sum, dv_sum
):
    group = pl.program_id(1)
    width = q_ref.shape[1]
    key_rows = group_columns(k_ref[...], group, groups)
    value_rows = group_columns(v_ref[...], group, groups)
    cosine, sine = cos_ref[...], sin_ref[...]
    dk_sum[...] = jnp.zeros_like(dk_sum)
    dv_sum[...] = jnp.zeros_like(dv_sum)
    for start in range(0, SEQ, QUERY_TILE):
        keys = start + QUERY_TILE
        bias, _ = tile_bias(row_ref, col_ref, start, QUERY_TILE, keys)
        grad_queries = []
        for head in range(width // HD):
            columns = slice(head * HD, (head + 1) * HD)
            query_tile = q_ref[start:keys, columns]
            grad_tile = grad_ref[start:keys, columns]
            probs = tile_probs(key_rows[:keys], query_tile, bias)
            grad_probs = contract_cols(value_rows[:keys], grad_tile)
            delta = jnp.sum(probs * grad_probs, axis=0, keepdims=True)
            grad_scores = (probs * (grad_probs - delta)).astype(jnp.bfloat16)
            dv_sum[:keys, :] += matmul(probs.astype(jnp.bfloat16), grad_tile)
            dk_sum[:keys, :] += matmul(grad_scores, query_tile)
            grad_queries.append(contract_rows(key_rows[:keys], grad_scores))
        turned = jnp.concatenate(grad_queries, axis=0).T * HD ** (-0.5)
        dq_ref[start:keys, :] = unrotate(
            turned, cosine[start:keys], sine[start:keys]
        ).astype(jnp.bfloat16)
    for own in range(groups):

        @pl.when(group == own)
        def _():
            columns = slice(own * HD, (own + 1) * HD)
            dk_ref[:, columns] = dk_sum[...] * HD ** (-0.5)
            dv_ref[:, columns] = dv_sum[...].astype(jnp.bfloat16)

    @pl.when(group == groups - 1)
    def _():
        narrow = dk_ref.shape[1]
        dk_ref[...] = unrotate(dk_ref[...], cosine[:, :narrow], sine[:, :narrow])


def attention_specs(rows, heads_width, keys_width):
    groups = keys_width // HD
    width = heads_width // groups
    grid = (rows // SEQ, groups)
    wide = pl.BlockSpec((SEQ, width), lambda s, g: (s, g))
    narrow = pl.BlockSpec((SEQ, keys_width), lambda s, g: (s, 0))
    docs = [
        pl.BlockSpec((1, 1, SEQ), lambda s, g: (s, 0, 0)),
        pl.BlockSpec((SEQ, 1), lambda s, g: (s, 0)),
    ]
    tables = [pl.BlockSpec((SEQ, width), lambda s, g: (0, 0))] * 2
    return groups, grid, wide, narrow, docs, tables


def attention_cost(rows, heads_width, matmuls):
    pairs = rows * SEQ * (heads_width // HD)
    return pl.CostEstimate(
        flops=2 * matmuls * pairs * HD, transcendentals=pairs, bytes_accessed=16 * rows * heads_width
    )


def attend(query_pre, key_pre, value_pre, doc_row, doc_col, tables):
    rows, heads_width = query_pre.shape
    keys_width = key_pre.shape[1]
    groups, grid, wide, narrow, docs, table_specs = attention_specs(rows, heads_width, keys_width)
    bf = jnp.bfloat16
    return pl.pallas_call(
        functools.partial(attend_kernel, groups),
        name="attend",
        grid=grid,
        in_specs=[wide, narrow, narrow] + docs + table_specs,
        out_specs=[wide, narrow, narrow, wide],
        out_shape=[
            jax.ShapeDtypeStruct((rows, heads_width), bf),
            jax.ShapeDtypeStruct((rows, keys_width), bf),
            jax.ShapeDtypeStruct((rows, keys_width), bf),
            jax.ShapeDtypeStruct((rows, heads_width), bf),
        ],
        cost_estimate=attention_cost(rows, heads_width, 2),
    )(query_pre, key_pre, value_pre, doc_row, doc_col, *tables)


def attend_back(query_rows, key_rows, value_rows, grad_mixed, doc_row, doc_col, tables):
    rows, heads_width = query_rows.shape
    keys_width = key_rows.shape[1]
    groups, grid, wide, narrow, docs, table_specs = attention_specs(rows, heads_width, keys_width)
    bf = jnp.bfloat16
    return pl.pallas_call(
        functools.partial(attend_back_kernel, groups),
        name="attend_back",
        grid=grid,
        in_specs=[wide, narrow, narrow, wide] + docs + table_specs,
        out_specs=[wide, narrow, narrow],
        out_shape=[
            jax.ShapeDtypeStruct((rows, heads_width), bf),
            jax.ShapeDtypeStruct((rows, keys_width), jnp.float32),
            jax.ShapeDtypeStruct((rows, keys_width), bf),
        ],
        scratch_shapes=[pltpu.VMEM((SEQ, HD), jnp.float32)] * 2,
        cost_estimate=attention_cost(rows, heads_width, 5),
    )(query_rows, key_rows, value_rows, grad_mixed, doc_row, doc_col, *tables)


def swap(array, axis, size, bit):
    return lax.ppermute(array, axis, [(i, i ^ bit) for i in range(size)])


def gather_rows(own, size):
    if size != 4:
        return lax.all_gather(own, "tensor", axis=0, tiled=True)
    me = lax.axis_index("tensor")
    rows = own.shape[0]
    half = rows // 2
    near_x = swap(own, "tensor", size, 1)
    near_y = swap(own, "tensor", size, 2)
    far_low = swap(near_x[:half], "tensor", size, 2)
    far_high = swap(near_y[half:], "tensor", size, 1)
    whole = jnp.zeros((size * rows,) + own.shape[1:], own.dtype)
    far = (me ^ 3) * rows
    for piece, at in (
        (own, me * rows),
        (near_x, (me ^ 1) * rows),
        (near_y, (me ^ 2) * rows),
        (far_low, far),
        (far_high, far + half),
    ):
        whole = lax.dynamic_update_slice_in_dim(whole, piece, at, 0)
    return whole


def sum_rows(partial, size):
    partial = partial.astype(jnp.bfloat16)
    if size != 4:
        return lax.psum_scatter(
            partial, "tensor", scatter_dimension=0, tiled=True
        ).astype(jnp.float32)
    me = lax.axis_index("tensor")
    rows = partial.shape[0] // size
    half = rows // 2

    def part(index, start=0, count=rows):
        return lax.dynamic_slice_in_dim(partial, index * rows + start, count, 0)

    from_x = swap(part(me ^ 3, 0, half), "tensor", size, 1)
    from_y = swap(part(me ^ 3, half, half), "tensor", size, 2)
    wide = jnp.float32
    to_y = jnp.concatenate(
        [
            (part(me ^ 2, 0, half).astype(wide) + from_x.astype(wide)).astype(jnp.bfloat16),
            part(me ^ 2, half, half),
        ]
    )
    to_x = jnp.concatenate(
        [
            part(me ^ 1, 0, half),
            (part(me ^ 1, half, half).astype(wide) + from_y.astype(wide)).astype(jnp.bfloat16),
        ]
    )
    last_y = swap(to_y, "tensor", size, 2)
    last_x = swap(to_x, "tensor", size, 1)
    return part(me).astype(wide) + last_x.astype(wide) + last_y.astype(wide)


def sum_all(array, axis, size):
    if size & (size - 1):
        return lax.psum(array, axis)
    bit = 1
    while bit < size:
        array = array + swap(array, axis, size, bit)
        bit *= 2
    return array


def parity_columns(rows, size):
    mine = lax.axis_index("dp") % 2
    cut = rows.reshape(rows.shape[0], size // 2, 2, rows.shape[1] // size)

    def pick(which):
        return lax.dynamic_index_in_dim(cut, which, 2, keepdims=False).reshape(rows.shape[0], -1)

    return pick(mine), pick(1 - mine)


def weight_grad(parities, right_side, size):
    mine, other = parities
    from_pair = swap(contract_rows(other, right_side).astype(jnp.bfloat16), "dp", size, 1)
    pair_sum = contract_rows(mine, right_side) + from_pair.astype(jnp.float32)
    groups = [list(range(0, size, 2)), list(range(1, size, 2))]
    return lax.psum_scatter(
        pair_sum.astype(jnp.bfloat16),
        "dp",
        scatter_dimension=0,
        tiled=True,
        axis_index_groups=groups,
    ).astype(jnp.float32)


def per_device(
    dp,
    tp,
    block_input,
    attn_gain,
    w_query,
    w_key,
    w_value,
    w_out,
    mlp_gain,
    w_gate,
    w_up,
    w_down,
    doc_ids,
    cotangent,
):
    heads_width, keys_width = w_query.shape[1], w_key.shape[1]
    splits = (heads_width, heads_width + keys_width)

    def gather(weight):
        return lax.all_gather(weight, "dp", axis=0, tiled=True)

    qkv_full = gather(jnp.concatenate([w_query, w_key, w_value], axis=1))
    out_full = gather(w_out)
    gate_full = gather(w_gate)
    up_full = gather(w_up)
    down_full = gather(w_down)

    live_all = (doc_ids >= 0).astype(jnp.float32)
    doc_row = doc_ids.reshape(-1, 1, SEQ)
    doc_col = doc_ids.reshape(-1, 1)
    tables = rotary_tables(SEQ, HD, heads_width // keys_width)

    input_own = block_input.astype(jnp.float32)
    scale_one = norm_scale(input_own)
    normed_one = gather_rows(
        (input_own * scale_one * attn_gain[None, :]).astype(jnp.bfloat16), tp
    )
    grad_full = gather_rows(cotangent, tp)

    qkv_pre = matmul(normed_one, qkv_full)
    query_rows, key_rows, value_rows, mixed_all = attend(
        *jnp.split(qkv_pre, splits, axis=1), doc_row, doc_col, tables
    )
    residual_own = input_own + sum_rows(contract_cols(mixed_all, out_full), tp)
    scale_two_own = norm_scale(residual_own)
    normed_two = gather_rows(
        (residual_own * scale_two_own * mlp_gain[None, :]).astype(jnp.bfloat16), tp
    )
    gate_pre = matmul(normed_two, gate_full)
    up_pre = matmul(normed_two, up_full)
    sigmoid_gate = jax.nn.sigmoid(gate_pre)
    silu_gate = gate_pre * sigmoid_gate
    hidden = (silu_gate * up_pre).astype(jnp.bfloat16)
    grad_down = weight_grad(parity_columns(grad_full, dp), hidden, dp)

    grad_hidden = matmul(grad_full, down_full)
    grad_gate_pre = (
        grad_hidden * up_pre * sigmoid_gate * (1.0 + gate_pre * (1.0 - sigmoid_gate))
    ).astype(jnp.bfloat16)
    grad_up_pre = (grad_hidden * silu_gate).astype(jnp.bfloat16)
    normed_two_parities = parity_columns(normed_two, dp)
    grad_gate = weight_grad(normed_two_parities, grad_gate_pre, dp)
    grad_up = weight_grad(normed_two_parities, grad_up_pre, dp)
    grad_normed_own = sum_rows(
        contract_cols(grad_gate_pre, gate_full) + contract_cols(grad_up_pre, up_full), tp
    )
    block_output = (residual_own + sum_rows(contract_cols(hidden, down_full), tp)).astype(
        jnp.bfloat16
    )
    grad_mlp_gain = jnp.sum(grad_normed_own * residual_own * scale_two_own, axis=0)
    grad_residual_own = cotangent.astype(jnp.float32) + norm_back(
        grad_normed_own, residual_own, scale_two_own, mlp_gain
    )
    grad_residual_bf = gather_rows(grad_residual_own.astype(jnp.bfloat16), tp)
    grad_out = weight_grad(parity_columns(grad_residual_bf, dp), mixed_all, dp)
    grad_mixed = (matmul(grad_residual_bf, out_full) * live_all[:, None]).astype(jnp.bfloat16)
    grad_query_rows, grad_keys, grad_value_rows = attend_back(
        query_rows, key_rows, value_rows, grad_mixed, doc_row, doc_col, tables
    )
    grad_qkv_rows = jnp.concatenate(
        [grad_query_rows, grad_keys.astype(jnp.bfloat16), grad_value_rows], axis=1
    )
    grad_qkv = weight_grad(parity_columns(normed_one, dp), grad_qkv_rows, dp)
    grad_query, grad_key, grad_value = jnp.split(grad_qkv, splits, axis=1)
    grad_normed_one = sum_rows(contract_cols(grad_qkv_rows, qkv_full), tp)
    grad_attn_gain = jnp.sum(grad_normed_one * input_own * scale_one, axis=0)
    input_grad = (
        grad_residual_own + norm_back(grad_normed_one, input_own, scale_one, attn_gain)
    ).astype(jnp.bfloat16)
    gains = jnp.stack([grad_attn_gain, grad_mlp_gain])
    gains = sum_all(sum_all(gains, "tensor", tp), "dp", dp)
    return (
        block_output,
        input_grad,
        grad_query,
        grad_key,
        grad_value,
        grad_out,
        grad_gate,
        grad_up,
        grad_down,
        gains[0],
        gains[1],
    )


def solution(mesh):
    in_specs = (
        P(("dp", "tensor"), None),
        P(),
        P("dp", "tensor"),
        P("dp", "tensor"),
        P("dp", "tensor"),
        P("dp", "tensor"),
        P(),
        P("dp", "tensor"),
        P("dp", "tensor"),
        P("dp", "tensor"),
        P("dp"),
        P(("dp", "tensor"), None),
    )
    out_specs = (
        P(("dp", "tensor"), None),
        P(("dp", "tensor"), None),
        P("dp", "tensor"),
        P("dp", "tensor"),
        P("dp", "tensor"),
        P("dp", "tensor"),
        P("dp", "tensor"),
        P("dp", "tensor"),
        P("dp", "tensor"),
        P(),
        P(),
    )
    return jax.shard_map(
        functools.partial(per_device, mesh.shape["dp"], mesh.shape["tensor"]),
        mesh=mesh,
        in_specs=in_specs,
        out_specs=out_specs,
        check_vma=False,
    )
```

```python
import functools

import jax
import jax.numpy as jnp
from jax import lax
from jax.experimental import pallas as pl
from jax.experimental.pallas import tpu as pltpu
from jax.sharding import PartitionSpec as P

HD = 64
SEQ = 512
QUERY_TILE = 256

EPSILON = 1e-05
ROPE_BASE = 500000.0
NEG_LARGE = -1e30


def rotary_tables(length, head_dim, copies):
    half_dim = head_dim // 2
    frequency = ROPE_BASE ** (-(jnp.arange(half_dim, dtype=jnp.float32) * (2.0 / head_dim)))
    angles = jnp.arange(length, dtype=jnp.float32)[:, None] * frequency[None, :]
    angles = jnp.concatenate([angles, angles] * copies, axis=1)
    return (jnp.cos(angles), jnp.sin(angles))


def norm_scale(tensor_rows):
    return lax.rsqrt(jnp.mean(tensor_rows * tensor_rows, axis=1, keepdims=True) + EPSILON)


def norm_back(grad_normed, tensor_rows, row_scale, gain_row):
    weighted = grad_normed * gain_row[None, :]
    inner_mean = jnp.mean(weighted * tensor_rows, axis=1, keepdims=True)
    return row_scale * weighted - tensor_rows * (row_scale * row_scale * row_scale) * inner_mean


def contract_rows(left_side, right_side):
    return lax.dot_general(
        left_side, right_side, (((0,), (0,)), ((), ())), preferred_element_type=jnp.float32
    )


def contract_cols(left_side, right_side):
    return lax.dot_general(
        left_side, right_side, (((1,), (1,)), ((), ())), preferred_element_type=jnp.float32
    )


def matmul(left_side, right_side):
    return jnp.dot(left_side, right_side, preferred_element_type=jnp.float32)


def half_turn(rows):
    width = rows.shape[1]
    first = lax.broadcasted_iota(jnp.int32, rows.shape, 1) % HD < HD // 2
    if width % 128 == 0:
        later = pltpu.roll(rows, width - HD // 2, axis=1)
        before = pltpu.roll(rows, HD // 2, axis=1)
        return jnp.where(first, later, before), first
    halves = [rows[:, at : at + HD // 2] for at in range(0, width, HD // 2)]
    swapped = [halves[i ^ 1] for i in range(len(halves))]
    return jnp.concatenate(swapped, axis=1), first


def rotate(rows, cosine, sine):
    turned, first = half_turn(rows)
    return rows * cosine + jnp.where(first, -turned, turned) * sine


def unrotate(rows, cosine, sine):
    turned, first = half_turn(rows * sine)
    return rows * cosine + jnp.where(first, turned, -turned)


def group_columns(rows, group, groups):
    picked = rows[:, :HD]
    for other in range(1, groups):
        picked = jnp.where(group == other, rows[:, other * HD : (other + 1) * HD], picked)
    return picked


def tile_bias(doc_row, doc_col, start, tile, keys):
    query_doc = doc_row[0, :, start : start + tile]
    key_doc = doc_col[:keys, :]
    key_at = lax.broadcasted_iota(jnp.int32, (keys, tile), 0)
    query_at = lax.broadcasted_iota(jnp.int32, (keys, tile), 1) + start
    same = (query_doc == key_doc) & (key_doc >= 0) & (key_at <= query_at)
    live = (query_doc >= 0).astype(jnp.float32)
    return jnp.where(same | (key_at == query_at), 0.0, NEG_LARGE), live


def tile_probs(keys_rows, query_tile, bias):
    scores = contract_cols(keys_rows, query_tile) * HD ** (-0.5) + bias
    weights = jnp.exp(scores - jnp.max(scores, axis=0, keepdims=True))
    return weights * (1.0 / jnp.sum(weights, axis=0, keepdims=True))


def attend_kernel(
    groups, q_ref, k_ref, v_ref, row_ref, col_ref, cos_ref, sin_ref,
    q_out, k_out, v_out, mixed_ref
):
    group = pl.program_id(1)
    width = q_ref.shape[1]
    narrow = k_ref.shape[1]
    query_rows = rotate(q_ref[...], cos_ref[...], sin_ref[...]).astype(jnp.bfloat16)
    key_all = rotate(k_ref[...], cos_ref[:, :narrow], sin_ref[:, :narrow]).astype(jnp.bfloat16)
    value_all = v_ref[...].astype(jnp.bfloat16)
    q_out[...] = query_rows
    k_out[...] = key_all
    v_out[...] = value_all
    key_rows = group_columns(key_all, group, groups)
    value_rows = group_columns(value_all, group, groups)
    for start in range(0, SEQ, QUERY_TILE):
        keys = start + QUERY_TILE
        bias, live = tile_bias(row_ref, col_ref, start, QUERY_TILE, keys)
        mixed = []
        for head in range(width // HD):
            query_tile = query_rows[start:keys, head * HD : (head + 1) * HD]
            probs = tile_probs(key_rows[:keys], query_tile, bias).astype(jnp.bfloat16)
            mixed.append(contract_rows(value_rows[:keys], probs) * live)
        mixed_ref[start:keys, :] = jnp.concatenate(mixed, axis=0).T.astype(jnp.bfloat16)


def attend_back_kernel(
    groups, q_ref, k_ref, v_ref, grad_ref, row_ref, col_ref, cos_ref, sin_ref,
    dq_ref, dk_ref, dv_ref, dk_sum, dv_sum
):
    group = pl.program_id(1)
    width = q_ref.shape[1]
    key_rows = group_columns(k_ref[...], group, groups)
    value_rows = group_columns(v_ref[...], group, groups)
    cosine, sine = cos_ref[...], sin_ref[...]
    dk_sum[...] = jnp.zeros_like(dk_sum)
    dv_sum[...] = jnp.zeros_like(dv_sum)
    for start in range(0, SEQ, QUERY_TILE):
        keys = start + QUERY_TILE
        bias, _ = tile_bias(row_ref, col_ref, start, QUERY_TILE, keys)
        grad_queries = []
        for head in range(width // HD):
            columns = slice(head * HD, (head + 1) * HD)
            query_tile = q_ref[start:keys, columns]
            grad_tile = grad_ref[start:keys, columns]
            probs = tile_probs(key_rows[:keys], query_tile, bias)
            grad_probs = contract_cols(value_rows[:keys], grad_tile)
            delta = jnp.sum(probs * grad_probs, axis=0, keepdims=True)
            grad_scores = (probs * (grad_probs - delta)).astype(jnp.bfloat16)
            dv_sum[:keys, :] += matmul(probs.astype(jnp.bfloat16), grad_tile)
            dk_sum[:keys, :] += matmul(grad_scores, query_tile)
            grad_queries.append(contract_rows(key_rows[:keys], grad_scores))
        turned = jnp.concatenate(grad_queries, axis=0).T * HD ** (-0.5)
        dq_ref[start:keys, :] = unrotate(
            turned, cosine[start:keys], sine[start:keys]
        ).astype(jnp.bfloat16)
    for own in range(groups):

        @pl.when(group == own)
        def _():
            columns = slice(own * HD, (own + 1) * HD)
            dk_ref[:, columns] = dk_sum[...] * HD ** (-0.5)
            dv_ref[:, columns] = dv_sum[...].astype(jnp.bfloat16)

    @pl.when(group == groups - 1)
    def _():
        narrow = dk_ref.shape[1]
        dk_ref[...] = unrotate(dk_ref[...], cosine[:, :narrow], sine[:, :narrow])


def attention_specs(rows, heads_width, keys_width):
    groups = keys_width // HD
    width = heads_width // groups
    grid = (rows // SEQ, groups)
    wide = pl.BlockSpec((SEQ, width), lambda s, g: (s, g))
    narrow = pl.BlockSpec((SEQ, keys_width), lambda s, g: (s, 0))
    docs = [
        pl.BlockSpec((1, 1, SEQ), lambda s, g: (s, 0, 0)),
        pl.BlockSpec((SEQ, 1), lambda s, g: (s, 0)),
    ]
    tables = [pl.BlockSpec((SEQ, width), lambda s, g: (0, 0))] * 2
    return groups, grid, wide, narrow, docs, tables


def attention_cost(rows, heads_width, matmuls):
    pairs = rows * SEQ * (heads_width // HD)
    return pl.CostEstimate(
        flops=2 * matmuls * pairs * HD, transcendentals=pairs, bytes_accessed=16 * rows * heads_width
    )


def attend(query_pre, key_pre, value_pre, doc_row, doc_col, tables):
    rows, heads_width = query_pre.shape
    keys_width = key_pre.shape[1]
    groups, grid, wide, narrow, docs, table_specs = attention_specs(rows, heads_width, keys_width)
    bf = jnp.bfloat16
    return pl.pallas_call(
        functools.partial(attend_kernel, groups),
        name="attend",
        grid=grid,
        in_specs=[wide, narrow, narrow] + docs + table_specs,
        out_specs=[wide, narrow, narrow, wide],
        out_shape=[
            jax.ShapeDtypeStruct((rows, heads_width), bf),
            jax.ShapeDtypeStruct((rows, keys_width), bf),
            jax.ShapeDtypeStruct((rows, keys_width), bf),
            jax.ShapeDtypeStruct((rows, heads_width), bf),
        ],
        cost_estimate=attention_cost(rows, heads_width, 2),
    )(query_pre, key_pre, value_pre, doc_row, doc_col, *tables)


def attend_back(query_rows, key_rows, value_rows, grad_mixed, doc_row, doc_col, tables):
    rows, heads_width = query_rows.shape
    keys_width = key_rows.shape[1]
    groups, grid, wide, narrow, docs, table_specs = attention_specs(rows, heads_width, keys_width)
    bf = jnp.bfloat16
    return pl.pallas_call(
        functools.partial(attend_back_kernel, groups),
        name="attend_back",
        grid=grid,
        in_specs=[wide, narrow, narrow, wide] + docs + table_specs,
        out_specs=[wide, narrow, narrow],
        out_shape=[
            jax.ShapeDtypeStruct((rows, heads_width), bf),
            jax.ShapeDtypeStruct((rows, keys_width), jnp.float32),
            jax.ShapeDtypeStruct((rows, keys_width), bf),
        ],
        scratch_shapes=[pltpu.VMEM((SEQ, HD), jnp.float32)] * 2,
        cost_estimate=attention_cost(rows, heads_width, 5),
    )(query_rows, key_rows, value_rows, grad_mixed, doc_row, doc_col, *tables)


def swap(array, axis, size, bit):
    return lax.ppermute(array, axis, [(i, i ^ bit) for i in range(size)])


def gather_rows(own, size):
    if size != 4:
        return lax.all_gather(own, "tensor", axis=0, tiled=True)
    me = lax.axis_index("tensor")
    rows = own.shape[0]
    half = rows // 2
    near_x = swap(own, "tensor", size, 1)
    near_y = swap(own, "tensor", size, 2)
    far_low = swap(near_x[:half], "tensor", size, 2)
    far_high = swap(near_y[half:], "tensor", size, 1)
    whole = jnp.zeros((size * rows,) + own.shape[1:], own.dtype)
    far = (me ^ 3) * rows
    for piece, at in (
        (own, me * rows),
        (near_x, (me ^ 1) * rows),
        (near_y, (me ^ 2) * rows),
        (far_low, far),
        (far_high, far + half),
    ):
        whole = lax.dynamic_update_slice_in_dim(whole, piece, at, 0)
    return whole


def sum_rows(partial, size):
    partial = partial.astype(jnp.bfloat16)
    if size != 4:
        return lax.psum_scatter(
            partial, "tensor", scatter_dimension=0, tiled=True
        ).astype(jnp.float32)
    me = lax.axis_index("tensor")
    rows = partial.shape[0] // size
    half = rows // 2

    def part(index, start=0, count=rows):
        return lax.dynamic_slice_in_dim(partial, index * rows + start, count, 0)

    from_x = swap(part(me ^ 3, 0, half), "tensor", size, 1)
    from_y = swap(part(me ^ 3, half, half), "tensor", size, 2)
    wide = jnp.float32
    to_y = jnp.concatenate(
        [
            (part(me ^ 2, 0, half).astype(wide) + from_x.astype(wide)).astype(jnp.bfloat16),
            part(me ^ 2, half, half),
        ]
    )
    to_x = jnp.concatenate(
        [
            part(me ^ 1, 0, half),
            (part(me ^ 1, half, half).astype(wide) + from_y.astype(wide)).astype(jnp.bfloat16),
        ]
    )
    last_y = swap(to_y, "tensor", size, 2)
    last_x = swap(to_x, "tensor", size, 1)
    return part(me).astype(wide) + last_x.astype(wide) + last_y.astype(wide)


def sum_all(array, axis, size):
    if size & (size - 1):
        return lax.psum(array, axis)
    bit = 1
    while bit < size:
        array = array + swap(array, axis, size, bit)
        bit *= 2
    return array


def parity_columns(rows, size):
    mine = lax.axis_index("dp") % 2
    cut = rows.reshape(rows.shape[0], size // 2, 2, rows.shape[1] // size)

    def pick(which):
        return lax.dynamic_index_in_dim(cut, which, 2, keepdims=False).reshape(rows.shape[0], -1)

    return pick(mine), pick(1 - mine)


def pair_grad(parities, right_side, size):
    mine, other = parities
    from_pair = swap(contract_rows(other, right_side).astype(jnp.bfloat16), "dp", size, 1)
    pair_sum = contract_rows(mine, right_side) + from_pair.astype(jnp.float32)
    return pair_sum.astype(jnp.bfloat16)


def sum_pairs(pair_sum, size):
    groups = [list(range(0, size, 2)), list(range(1, size, 2))]
    return lax.psum_scatter(
        pair_sum,
        "dp",
        scatter_dimension=0,
        tiled=True,
        axis_index_groups=groups,
    ).astype(jnp.float32)


def per_device(
    dp,
    tp,
    block_input,
    attn_gain,
    w_query,
    w_key,
    w_value,
    w_out,
    mlp_gain,
    w_gate,
    w_up,
    w_down,
    doc_ids,
    cotangent,
):
    heads_width, keys_width = w_query.shape[1], w_key.shape[1]
    splits = (heads_width, heads_width + keys_width)

    def gather(weight):
        return lax.all_gather(weight, "dp", axis=0, tiled=True)

    qkv_full = gather(jnp.concatenate([w_query, w_key, w_value], axis=1))
    out_full = gather(w_out)
    gate_full = gather(w_gate)
    up_full = gather(w_up)
    down_full = gather(w_down)

    live_all = (doc_ids >= 0).astype(jnp.float32)
    doc_row = doc_ids.reshape(-1, 1, SEQ)
    doc_col = doc_ids.reshape(-1, 1)
    tables = rotary_tables(SEQ, HD, heads_width // keys_width)

    input_own = block_input.astype(jnp.float32)
    scale_one = norm_scale(input_own)
    normed_one = gather_rows(
        (input_own * scale_one * attn_gain[None, :]).astype(jnp.bfloat16), tp
    )
    grad_full = gather_rows(cotangent, tp)

    qkv_pre = matmul(normed_one, qkv_full)
    query_rows, key_rows, value_rows, mixed_all = attend(
        *jnp.split(qkv_pre, splits, axis=1), doc_row, doc_col, tables
    )
    residual_own = input_own + sum_rows(contract_cols(mixed_all, out_full), tp)
    scale_two_own = norm_scale(residual_own)
    normed_two = gather_rows(
        (residual_own * scale_two_own * mlp_gain[None, :]).astype(jnp.bfloat16), tp
    )
    gate_pre = matmul(normed_two, gate_full)
    up_pre = matmul(normed_two, up_full)
    sigmoid_gate = jax.nn.sigmoid(gate_pre)
    silu_gate = gate_pre * sigmoid_gate
    hidden = (silu_gate * up_pre).astype(jnp.bfloat16)
    pair_down = pair_grad(parity_columns(grad_full, dp), hidden, dp)
    pair_down, down_full = lax.optimization_barrier((pair_down, down_full))
    grad_down = sum_pairs(pair_down, dp)

    grad_hidden = matmul(grad_full, down_full)
    grad_gate_pre = (
        grad_hidden * up_pre * sigmoid_gate * (1.0 + gate_pre * (1.0 - sigmoid_gate))
    ).astype(jnp.bfloat16)
    grad_up_pre = (grad_hidden * silu_gate).astype(jnp.bfloat16)
    grad_normed_part = (
        contract_cols(grad_gate_pre, gate_full) + contract_cols(grad_up_pre, up_full)
    ).astype(jnp.bfloat16)
    grad_normed_part, grad_gate_pre, grad_up_pre = lax.optimization_barrier(
        (grad_normed_part, grad_gate_pre, grad_up_pre)
    )
    normed_two_parities = parity_columns(normed_two, dp)
    pair_gate = pair_grad(normed_two_parities, grad_gate_pre, dp)
    pair_up = pair_grad(normed_two_parities, grad_up_pre, dp)
    grad_normed_own = sum_rows(grad_normed_part, tp)
    grad_normed_own, pair_gate, pair_up = lax.optimization_barrier(
        (grad_normed_own, pair_gate, pair_up)
    )
    grad_gate = sum_pairs(pair_gate, dp)
    grad_up = sum_pairs(pair_up, dp)
    grad_mlp_gain = jnp.sum(grad_normed_own * residual_own * scale_two_own, axis=0)
    grad_residual_own = cotangent.astype(jnp.float32) + norm_back(
        grad_normed_own, residual_own, scale_two_own, mlp_gain
    )
    grad_residual_bf = gather_rows(grad_residual_own.astype(jnp.bfloat16), tp)
    grad_residual_bf, hidden = lax.optimization_barrier((grad_residual_bf, hidden))
    grad_mixed = (matmul(grad_residual_bf, out_full) * live_all[:, None]).astype(jnp.bfloat16)
    block_output = (residual_own + sum_rows(contract_cols(hidden, down_full), tp)).astype(
        jnp.bfloat16
    )
    grad_query_rows, grad_keys, grad_value_rows = attend_back(
        query_rows, key_rows, value_rows, grad_mixed, doc_row, doc_col, tables
    )
    grad_qkv_rows = jnp.concatenate(
        [grad_query_rows, grad_keys.astype(jnp.bfloat16), grad_value_rows], axis=1
    )
    grad_one_part = contract_cols(grad_qkv_rows, qkv_full).astype(jnp.bfloat16)
    grad_one_part, grad_qkv_rows, mixed_all = lax.optimization_barrier(
        (grad_one_part, grad_qkv_rows, mixed_all)
    )
    pair_out = pair_grad(parity_columns(grad_residual_bf, dp), mixed_all, dp)
    pair_qkv = pair_grad(parity_columns(normed_one, dp), grad_qkv_rows, dp)
    grad_out = sum_pairs(pair_out, dp)
    grad_qkv = sum_pairs(pair_qkv, dp)
    grad_query, grad_key, grad_value = jnp.split(grad_qkv, splits, axis=1)
    grad_normed_one = sum_rows(grad_one_part, tp)
    grad_attn_gain = jnp.sum(grad_normed_one * input_own * scale_one, axis=0)
    input_grad = (
        grad_residual_own + norm_back(grad_normed_one, input_own, scale_one, attn_gain)
    ).astype(jnp.bfloat16)
    gains = jnp.stack([grad_attn_gain, grad_mlp_gain])
    gains = sum_all(sum_all(gains, "tensor", tp), "dp", dp)
    return (
        block_output,
        input_grad,
        grad_query,
        grad_key,
        grad_value,
        grad_out,
        grad_gate,
        grad_up,
        grad_down,
        gains[0],
        gains[1],
    )


def solution(mesh):
    in_specs = (
        P(("dp", "tensor"), None),
        P(),
        P("dp", "tensor"),
        P("dp", "tensor"),
        P("dp", "tensor"),
        P("dp", "tensor"),
        P(),
        P("dp", "tensor"),
        P("dp", "tensor"),
        P("dp", "tensor"),
        P("dp"),
        P(("dp", "tensor"), None),
    )
    out_specs = (
        P(("dp", "tensor"), None),
        P(("dp", "tensor"), None),
        P("dp", "tensor"),
        P("dp", "tensor"),
        P("dp", "tensor"),
        P("dp", "tensor"),
        P("dp", "tensor"),
        P("dp", "tensor"),
        P("dp", "tensor"),
        P(),
        P(),
    )
    return jax.shard_map(
        functools.partial(per_device, mesh.shape["dp"], mesh.shape["tensor"]),
        mesh=mesh,
        in_specs=in_specs,
        out_specs=out_specs,
        check_vma=False,
    )
```

```python
import functools

import jax
import jax.numpy as jnp
from jax import lax
from jax.experimental import pallas as pl
from jax.experimental.pallas import tpu as pltpu
from jax.sharding import PartitionSpec as P


HD = 64
SEQ = 512
QUERY_TILE = 256

EPSILON = 1e-05
ROPE_BASE = 500000.0
NEG_LARGE = -1e30


def rotary_tables(length, head_dim, copies):
    half_dim = head_dim // 2
    frequency = ROPE_BASE ** (-(jnp.arange(half_dim, dtype=jnp.float32) * (2.0 / head_dim)))
    angles = jnp.arange(length, dtype=jnp.float32)[:, None] * frequency[None, :]
    angles = jnp.concatenate([angles, angles] * copies, axis=1)
    return (jnp.cos(angles), jnp.sin(angles))


def norm_scale(tensor_rows):
    return lax.rsqrt(jnp.mean(tensor_rows * tensor_rows, axis=1, keepdims=True) + EPSILON)


def norm_back(grad_normed, tensor_rows, row_scale, gain_row):
    weighted = grad_normed * gain_row[None, :]
    inner_mean = jnp.mean(weighted * tensor_rows, axis=1, keepdims=True)
    return row_scale * weighted - tensor_rows * (row_scale * row_scale * row_scale) * inner_mean


def contract_rows(left_side, right_side):
    return lax.dot_general(
        left_side, right_side, (((0,), (0,)), ((), ())), preferred_element_type=jnp.float32
    )


def contract_cols(left_side, right_side):
    return lax.dot_general(
        left_side, right_side, (((1,), (1,)), ((), ())), preferred_element_type=jnp.float32
    )


def matmul(left_side, right_side):
    return jnp.dot(left_side, right_side, preferred_element_type=jnp.float32)


def half_turn(rows):
    width = rows.shape[1]
    first = lax.broadcasted_iota(jnp.int32, rows.shape, 1) % HD < HD // 2
    if width % 128 == 0:
        later = pltpu.roll(rows, width - HD // 2, axis=1)
        before = pltpu.roll(rows, HD // 2, axis=1)
        return jnp.where(first, later, before), first
    halves = [rows[:, at : at + HD // 2] for at in range(0, width, HD // 2)]
    swapped = [halves[i ^ 1] for i in range(len(halves))]
    return jnp.concatenate(swapped, axis=1), first


def rotate(rows, cosine, sine):
    turned, first = half_turn(rows)
    return rows * cosine + jnp.where(first, -turned, turned) * sine


def unrotate(rows, cosine, sine):
    turned, first = half_turn(rows * sine)
    return rows * cosine + jnp.where(first, turned, -turned)


def group_columns(rows, group, groups):
    picked = rows[:, :HD]
    for other in range(1, groups):
        picked = jnp.where(group == other, rows[:, other * HD : (other + 1) * HD], picked)
    return picked


def tile_bias(doc_row, doc_col, start, tile, keys):
    query_doc = doc_row[0, :, start : start + tile]
    key_doc = doc_col[:keys, :]
    key_at = lax.broadcasted_iota(jnp.int32, (keys, tile), 0)
    query_at = lax.broadcasted_iota(jnp.int32, (keys, tile), 1) + start
    same = (query_doc == key_doc) & (key_doc >= 0) & (key_at <= query_at)
    live = (query_doc >= 0).astype(jnp.float32)
    return jnp.where(same | (key_at == query_at), 0.0, NEG_LARGE), live


def tile_probs(keys_rows, query_tile, bias):
    scores = contract_cols(keys_rows, query_tile) * HD ** (-0.5) + bias
    weights = jnp.exp(scores - jnp.max(scores, axis=0, keepdims=True))
    return weights * (1.0 / jnp.sum(weights, axis=0, keepdims=True))


def attend_kernel(
    groups, q_ref, k_ref, v_ref, row_ref, col_ref, cos_ref, sin_ref,
    q_out, k_out, v_out, mixed_ref
):
    group = pl.program_id(1)
    width = q_ref.shape[1]
    narrow = k_ref.shape[1]
    query_rows = rotate(q_ref[...], cos_ref[...], sin_ref[...]).astype(jnp.bfloat16)
    key_all = rotate(k_ref[...], cos_ref[:, :narrow], sin_ref[:, :narrow]).astype(jnp.bfloat16)
    value_all = v_ref[...].astype(jnp.bfloat16)
    q_out[...] = query_rows
    k_out[...] = key_all
    v_out[...] = value_all
    key_rows = group_columns(key_all, group, groups)
    value_rows = group_columns(value_all, group, groups)
    for start in range(0, SEQ, QUERY_TILE):
        keys = start + QUERY_TILE
        bias, live = tile_bias(row_ref, col_ref, start, QUERY_TILE, keys)
        mixed = []
        for head in range(width // HD):
            query_tile = query_rows[start:keys, head * HD : (head + 1) * HD]
            probs = tile_probs(key_rows[:keys], query_tile, bias).astype(jnp.bfloat16)
            mixed.append(contract_rows(value_rows[:keys], probs) * live)
        mixed_ref[start:keys, :] = jnp.concatenate(mixed, axis=0).T.astype(jnp.bfloat16)


def attend_back_kernel(
    groups, q_ref, k_ref, v_ref, grad_ref, row_ref, col_ref, cos_ref, sin_ref,
    dq_ref, dk_ref, dv_ref, dk_sum, dv_sum
):
    group = pl.program_id(1)
    width = q_ref.shape[1]
    key_rows = group_columns(k_ref[...], group, groups)
    value_rows = group_columns(v_ref[...], group, groups)
    cosine, sine = cos_ref[...], sin_ref[...]
    dk_sum[...] = jnp.zeros_like(dk_sum)
    dv_sum[...] = jnp.zeros_like(dv_sum)
    for start in range(0, SEQ, QUERY_TILE):
        keys = start + QUERY_TILE
        bias, _ = tile_bias(row_ref, col_ref, start, QUERY_TILE, keys)
        grad_queries = []
        for head in range(width // HD):
            columns = slice(head * HD, (head + 1) * HD)
            query_tile = q_ref[start:keys, columns]
            grad_tile = grad_ref[start:keys, columns]
            probs = tile_probs(key_rows[:keys], query_tile, bias)
            grad_probs = contract_cols(value_rows[:keys], grad_tile)
            delta = jnp.sum(probs * grad_probs, axis=0, keepdims=True)
            grad_scores = (probs * (grad_probs - delta)).astype(jnp.bfloat16)
            dv_sum[:keys, :] += matmul(probs.astype(jnp.bfloat16), grad_tile)
            dk_sum[:keys, :] += matmul(grad_scores, query_tile)
            grad_queries.append(contract_rows(key_rows[:keys], grad_scores))
        turned = jnp.concatenate(grad_queries, axis=0).T * HD ** (-0.5)
        dq_ref[start:keys, :] = unrotate(
            turned, cosine[start:keys], sine[start:keys]
        ).astype(jnp.bfloat16)
    for own in range(groups):

        @pl.when(group == own)
        def _():
            columns = slice(own * HD, (own + 1) * HD)
            dk_ref[:, columns] = dk_sum[...] * HD ** (-0.5)
            dv_ref[:, columns] = dv_sum[...].astype(jnp.bfloat16)

    @pl.when(group == groups - 1)
    def _():
        narrow = dk_ref.shape[1]
        dk_ref[...] = unrotate(dk_ref[...], cosine[:, :narrow], sine[:, :narrow])


def attention_specs(rows, heads_width, keys_width):
    groups = keys_width // HD
    width = heads_width // groups
    grid = (rows // SEQ, groups)
    wide = pl.BlockSpec((SEQ, width), lambda s, g: (s, g))
    narrow = pl.BlockSpec((SEQ, keys_width), lambda s, g: (s, 0))
    docs = [
        pl.BlockSpec((1, 1, SEQ), lambda s, g: (s, 0, 0)),
        pl.BlockSpec((SEQ, 1), lambda s, g: (s, 0)),
    ]
    tables = [pl.BlockSpec((SEQ, width), lambda s, g: (0, 0))] * 2
    return groups, grid, wide, narrow, docs, tables


def attention_cost(rows, heads_width, matmuls):
    pairs = rows * SEQ * (heads_width // HD)
    return pl.CostEstimate(
        flops=2 * matmuls * pairs * HD, transcendentals=pairs, bytes_accessed=16 * rows * heads_width
    )


def attend(query_pre, key_pre, value_pre, doc_row, doc_col, tables):
    rows, heads_width = query_pre.shape
    keys_width = key_pre.shape[1]
    groups, grid, wide, narrow, docs, table_specs = attention_specs(rows, heads_width, keys_width)
    bf = jnp.bfloat16
    return pl.pallas_call(
        functools.partial(attend_kernel, groups),
        name="attend",
        grid=grid,
        in_specs=[wide, narrow, narrow] + docs + table_specs,
        out_specs=[wide, narrow, narrow, wide],
        out_shape=[
            jax.ShapeDtypeStruct((rows, heads_width), bf),
            jax.ShapeDtypeStruct((rows, keys_width), bf),
            jax.ShapeDtypeStruct((rows, keys_width), bf),
            jax.ShapeDtypeStruct((rows, heads_width), bf),
        ],
        cost_estimate=attention_cost(rows, heads_width, 2),
    )(query_pre, key_pre, value_pre, doc_row, doc_col, *tables)


def attend_back(query_rows, key_rows, value_rows, grad_mixed, doc_row, doc_col, tables):
    rows, heads_width = query_rows.shape
    keys_width = key_rows.shape[1]
    groups, grid, wide, narrow, docs, table_specs = attention_specs(rows, heads_width, keys_width)
    bf = jnp.bfloat16
    return pl.pallas_call(
        functools.partial(attend_back_kernel, groups),
        name="attend_back",
        grid=grid,
        in_specs=[wide, narrow, narrow, wide] + docs + table_specs,
        out_specs=[wide, narrow, narrow],
        out_shape=[
            jax.ShapeDtypeStruct((rows, heads_width), bf),
            jax.ShapeDtypeStruct((rows, keys_width), jnp.float32),
            jax.ShapeDtypeStruct((rows, keys_width), bf),
        ],
        scratch_shapes=[pltpu.VMEM((SEQ, HD), jnp.float32)] * 2,
        cost_estimate=attention_cost(rows, heads_width, 5),
    )(query_rows, key_rows, value_rows, grad_mixed, doc_row, doc_col, *tables)


def swap(array, axis, size, bit):
    return lax.ppermute(array, axis, [(i, i ^ bit) for i in range(size)])


def gather_rows(own, size):
    if size != 4:
        return lax.all_gather(own, "tensor", axis=0, tiled=True)
    me = lax.axis_index("tensor")
    rows = own.shape[0]
    half = rows // 2
    near_x = swap(own, "tensor", size, 1)
    near_y = swap(own, "tensor", size, 2)
    far_low = swap(near_x[:half], "tensor", size, 2)
    far_high = swap(near_y[half:], "tensor", size, 1)
    whole = jnp.zeros((size * rows,) + own.shape[1:], own.dtype)
    far = (me ^ 3) * rows
    for piece, at in (
        (own, me * rows),
        (near_x, (me ^ 1) * rows),
        (near_y, (me ^ 2) * rows),
        (far_low, far),
        (far_high, far + half),
    ):
        whole = lax.dynamic_update_slice_in_dim(whole, piece, at, 0)
    return whole


def sum_rows(partial, size):
    partial = partial.astype(jnp.bfloat16)
    if size != 4:
        return lax.psum_scatter(
            partial, "tensor", scatter_dimension=0, tiled=True
        ).astype(jnp.float32)
    me = lax.axis_index("tensor")
    rows = partial.shape[0] // size
    half = rows // 2

    def part(index, start=0, count=rows):
        return lax.dynamic_slice_in_dim(partial, index * rows + start, count, 0)

    from_x = swap(part(me ^ 3, 0, half), "tensor", size, 1)
    from_y = swap(part(me ^ 3, half, half), "tensor", size, 2)
    wide = jnp.float32
    to_y = jnp.concatenate(
        [
            (part(me ^ 2, 0, half).astype(wide) + from_x.astype(wide)).astype(jnp.bfloat16),
            part(me ^ 2, half, half),
        ]
    )
    to_x = jnp.concatenate(
        [
            part(me ^ 1, 0, half),
            (part(me ^ 1, half, half).astype(wide) + from_y.astype(wide)).astype(jnp.bfloat16),
        ]
    )
    last_y = swap(to_y, "tensor", size, 2)
    last_x = swap(to_x, "tensor", size, 1)
    return part(me).astype(wide) + last_x.astype(wide) + last_y.astype(wide)


def sum_all(array, axis, size):
    if size & (size - 1):
        return lax.psum(array, axis)
    bit = 1
    while bit < size:
        array = array + swap(array, axis, size, bit)
        bit *= 2
    return array


def parity_columns(rows, size):
    mine = lax.axis_index("dp") % 2
    cut = rows.reshape(rows.shape[0], size // 2, 2, rows.shape[1] // size)

    def pick(which):
        return lax.dynamic_index_in_dim(cut, which, 2, keepdims=False).reshape(rows.shape[0], -1)

    return pick(mine), pick(1 - mine)


def pair_grad(parities, right_side, size):
    mine, other = parities
    from_pair = swap(contract_rows(other, right_side).astype(jnp.bfloat16), "dp", size, 1)
    pair_sum = contract_rows(mine, right_side) + from_pair.astype(jnp.float32)
    return pair_sum.astype(jnp.bfloat16)


def sum_pairs(pair_sum, size):
    groups = [list(range(0, size, 2)), list(range(1, size, 2))]
    return lax.psum_scatter(
        pair_sum,
        "dp",
        scatter_dimension=0,
        tiled=True,
        axis_index_groups=groups,
    ).astype(jnp.float32)


def per_device(
    dp,
    tp,
    block_input,
    attn_gain,
    w_query,
    w_key,
    w_value,
    w_out,
    mlp_gain,
    w_gate,
    w_up,
    w_down,
    doc_ids,
    cotangent,
):
    heads_width, keys_width = w_query.shape[1], w_key.shape[1]
    splits = (heads_width, heads_width + keys_width)

    def gather(weight):
        return lax.all_gather(weight, "dp", axis=0, tiled=True)

    narrow = splits[1] + keys_width
    small_full = gather(jnp.concatenate([w_query, w_key, w_value, w_out], axis=1))
    qkv_full, out_full = small_full[:, :narrow], small_full[:, narrow:]
    gate_full, up_full = jnp.split(gather(jnp.concatenate([w_gate, w_up], axis=1)), 2, axis=1)
    down_full = gather(w_down)

    live_all = (doc_ids >= 0).astype(jnp.float32)
    doc_row = doc_ids.reshape(-1, 1, SEQ)
    doc_col = doc_ids.reshape(-1, 1)
    tables = rotary_tables(SEQ, HD, heads_width // keys_width)

    input_own = block_input.astype(jnp.float32)
    scale_one = norm_scale(input_own)
    normed_one = gather_rows(
        (input_own * scale_one * attn_gain[None, :]).astype(jnp.bfloat16), tp
    )
    grad_full = gather_rows(cotangent, tp)

    qkv_pre = matmul(normed_one, qkv_full)
    query_rows, key_rows, value_rows, mixed_all = attend(
        *jnp.split(qkv_pre, splits, axis=1), doc_row, doc_col, tables
    )
    residual_own = input_own + sum_rows(contract_cols(mixed_all, out_full), tp)
    scale_two_own = norm_scale(residual_own)
    normed_two = gather_rows(
        (residual_own * scale_two_own * mlp_gain[None, :]).astype(jnp.bfloat16), tp
    )
    gate_pre = matmul(normed_two, gate_full)
    up_pre = matmul(normed_two, up_full)
    sigmoid_gate = jax.nn.sigmoid(gate_pre)
    silu_gate = gate_pre * sigmoid_gate
    hidden = (silu_gate * up_pre).astype(jnp.bfloat16)
    pair_down = pair_grad(parity_columns(grad_full, dp), hidden, dp)
    one_parities = parity_columns(normed_one, dp)
    two_parities = parity_columns(normed_two, dp)
    pair_down, down_full, one_parities, two_parities = lax.optimization_barrier(
        (pair_down, down_full, one_parities, two_parities)
    )
    grad_down = sum_pairs(pair_down, dp)

    grad_hidden = matmul(grad_full, down_full)
    grad_gate_pre = (
        grad_hidden * up_pre * sigmoid_gate * (1.0 + gate_pre * (1.0 - sigmoid_gate))
    ).astype(jnp.bfloat16)
    grad_up_pre = (grad_hidden * silu_gate).astype(jnp.bfloat16)
    grad_normed_part = (
        contract_cols(grad_gate_pre, gate_full) + contract_cols(grad_up_pre, up_full)
    ).astype(jnp.bfloat16)
    grad_normed_part, grad_gate_pre, grad_up_pre = lax.optimization_barrier(
        (grad_normed_part, grad_gate_pre, grad_up_pre)
    )
    pair_gate_up = jnp.concatenate(
        [pair_grad(two_parities, grad_gate_pre, dp), pair_grad(two_parities, grad_up_pre, dp)],
        axis=1,
    )
    grad_normed_own = sum_rows(grad_normed_part, tp)
    grad_normed_own, pair_gate_up = lax.optimization_barrier((grad_normed_own, pair_gate_up))
    grad_gate, grad_up = jnp.split(sum_pairs(pair_gate_up, dp), 2, axis=1)
    grad_mlp_gain = jnp.sum(grad_normed_own * residual_own * scale_two_own, axis=0)
    grad_residual_own = cotangent.astype(jnp.float32) + norm_back(
        grad_normed_own, residual_own, scale_two_own, mlp_gain
    )
    grad_residual_bf = gather_rows(grad_residual_own.astype(jnp.bfloat16), tp)
    grad_residual_bf, hidden = lax.optimization_barrier((grad_residual_bf, hidden))
    grad_mixed = (matmul(grad_residual_bf, out_full) * live_all[:, None]).astype(jnp.bfloat16)
    block_output = (residual_own + sum_rows(contract_cols(hidden, down_full), tp)).astype(
        jnp.bfloat16
    )
    grad_query_rows, grad_keys, grad_value_rows = attend_back(
        query_rows, key_rows, value_rows, grad_mixed, doc_row, doc_col, tables
    )
    grad_qkv_rows = jnp.concatenate(
        [grad_query_rows, grad_keys.astype(jnp.bfloat16), grad_value_rows], axis=1
    )
    grad_one_part = contract_cols(grad_qkv_rows, qkv_full).astype(jnp.bfloat16)
    grad_one_part, grad_qkv_rows, mixed_all = lax.optimization_barrier(
        (grad_one_part, grad_qkv_rows, mixed_all)
    )
    pair_small = jnp.concatenate(
        [
            pair_grad(one_parities, grad_qkv_rows, dp),
            pair_grad(parity_columns(grad_residual_bf, dp), mixed_all, dp),
        ],
        axis=1,
    )
    grad_query, grad_key, grad_value, grad_out = jnp.split(
        sum_pairs(pair_small, dp), splits + (narrow,), axis=1
    )
    grad_normed_one = sum_rows(grad_one_part, tp)
    grad_attn_gain = jnp.sum(grad_normed_one * input_own * scale_one, axis=0)
    input_grad = (
        grad_residual_own + norm_back(grad_normed_one, input_own, scale_one, attn_gain)
    ).astype(jnp.bfloat16)
    gains = jnp.stack([grad_attn_gain, grad_mlp_gain])
    gains = sum_all(sum_all(gains, "tensor", tp), "dp", dp)
    return (
        block_output,
        input_grad,
        grad_query,
        grad_key,
        grad_value,
        grad_out,
        grad_gate,
        grad_up,
        grad_down,
        gains[0],
        gains[1],
    )


def solution(mesh):
    in_specs = (
        P(("dp", "tensor"), None),
        P(),
        P("dp", "tensor"),
        P("dp", "tensor"),
        P("dp", "tensor"),
        P("dp", "tensor"),
        P(),
        P("dp", "tensor"),
        P("dp", "tensor"),
        P("dp", "tensor"),
        P("dp"),
        P(("dp", "tensor"), None),
    )
    out_specs = (
        P(("dp", "tensor"), None),
        P(("dp", "tensor"), None),
        P("dp", "tensor"),
        P("dp", "tensor"),
        P("dp", "tensor"),
        P("dp", "tensor"),
        P("dp", "tensor"),
        P("dp", "tensor"),
        P("dp", "tensor"),
        P(),
        P(),
    )
    return jax.shard_map(
        functools.partial(per_device, mesh.shape["dp"], mesh.shape["tensor"]),
        mesh=mesh,
        in_specs=in_specs,
        out_specs=out_specs,
        check_vma=False,
    )
```

```python
import functools

import jax
import jax.numpy as jnp
from jax import lax
from jax.experimental import pallas as pl
from jax.experimental.pallas import tpu as pltpu
from jax.sharding import PartitionSpec as P


HD = 64
SEQ = 512
QUERY_TILE = 256

EPSILON = 1e-05
ROPE_BASE = 500000.0
NEG_LARGE = -1e30


def rotary_tables(length, head_dim, copies):
    half_dim = head_dim // 2
    frequency = ROPE_BASE ** (-(jnp.arange(half_dim, dtype=jnp.float32) * (2.0 / head_dim)))
    angles = jnp.arange(length, dtype=jnp.float32)[:, None] * frequency[None, :]
    angles = jnp.concatenate([angles, angles] * copies, axis=1)
    return (jnp.cos(angles), jnp.sin(angles))


def norm_scale(tensor_rows):
    return lax.rsqrt(jnp.mean(tensor_rows * tensor_rows, axis=1, keepdims=True) + EPSILON)


def norm_back(grad_normed, tensor_rows, row_scale, gain_row):
    weighted = grad_normed * gain_row[None, :]
    inner_mean = jnp.mean(weighted * tensor_rows, axis=1, keepdims=True)
    return row_scale * weighted - tensor_rows * (row_scale * row_scale * row_scale) * inner_mean


def contract_rows(left_side, right_side):
    return lax.dot_general(
        left_side, right_side, (((0,), (0,)), ((), ())), preferred_element_type=jnp.float32
    )


def contract_cols(left_side, right_side):
    return lax.dot_general(
        left_side, right_side, (((1,), (1,)), ((), ())), preferred_element_type=jnp.float32
    )


def matmul(left_side, right_side):
    return jnp.dot(left_side, right_side, preferred_element_type=jnp.float32)


def half_turn(rows):
    width = rows.shape[1]
    first = lax.broadcasted_iota(jnp.int32, rows.shape, 1) % HD < HD // 2
    if width % 128 == 0:
        later = pltpu.roll(rows, width - HD // 2, axis=1)
        before = pltpu.roll(rows, HD // 2, axis=1)
        return jnp.where(first, later, before), first
    halves = [rows[:, at : at + HD // 2] for at in range(0, width, HD // 2)]
    swapped = [halves[i ^ 1] for i in range(len(halves))]
    return jnp.concatenate(swapped, axis=1), first


def rotate(rows, cosine, sine):
    turned, first = half_turn(rows)
    return rows * cosine + jnp.where(first, -turned, turned) * sine


def unrotate(rows, cosine, sine):
    turned, first = half_turn(rows * sine)
    return rows * cosine + jnp.where(first, turned, -turned)


def group_columns(rows, group, groups):
    picked = rows[:, :HD]
    for other in range(1, groups):
        picked = jnp.where(group == other, rows[:, other * HD : (other + 1) * HD], picked)
    return picked


def tile_bias(doc_row, doc_col, start, tile, keys):
    query_doc = doc_row[0, :, start : start + tile]
    key_doc = doc_col[:keys, :]
    key_at = lax.broadcasted_iota(jnp.int32, (keys, tile), 0)
    query_at = lax.broadcasted_iota(jnp.int32, (keys, tile), 1) + start
    same = (query_doc == key_doc) & (key_doc >= 0) & (key_at <= query_at)
    live = (query_doc >= 0).astype(jnp.float32)
    return jnp.where(same | (key_at == query_at), 0.0, NEG_LARGE), live


def tile_probs(keys_rows, query_tile, bias):
    scores = contract_cols(keys_rows, query_tile) * HD ** (-0.5) + bias
    weights = jnp.exp(scores - jnp.max(scores, axis=0, keepdims=True))
    return weights * (1.0 / jnp.sum(weights, axis=0, keepdims=True))


def attend_kernel(
    groups, q_ref, k_ref, v_ref, row_ref, col_ref, cos_ref, sin_ref,
    q_out, k_out, v_out, mixed_ref
):
    group = pl.program_id(1)
    width = q_ref.shape[1]
    narrow = k_ref.shape[1]
    query_rows = rotate(q_ref[...], cos_ref[...], sin_ref[...]).astype(jnp.bfloat16)
    key_all = rotate(k_ref[...], cos_ref[:, :narrow], sin_ref[:, :narrow]).astype(jnp.bfloat16)
    value_all = v_ref[...].astype(jnp.bfloat16)
    q_out[...] = query_rows
    k_out[...] = key_all
    v_out[...] = value_all
    key_rows = group_columns(key_all, group, groups)
    value_rows = group_columns(value_all, group, groups)
    for start in range(0, SEQ, QUERY_TILE):
        keys = start + QUERY_TILE
        bias, live = tile_bias(row_ref, col_ref, start, QUERY_TILE, keys)
        mixed = []
        for head in range(width // HD):
            query_tile = query_rows[start:keys, head * HD : (head + 1) * HD]
            probs = tile_probs(key_rows[:keys], query_tile, bias).astype(jnp.bfloat16)
            mixed.append(contract_rows(value_rows[:keys], probs) * live)
        mixed_ref[start:keys, :] = jnp.concatenate(mixed, axis=0).T.astype(jnp.bfloat16)


def attend_back_kernel(
    groups, q_ref, k_ref, v_ref, grad_ref, row_ref, col_ref, cos_ref, sin_ref,
    dq_ref, dk_ref, dv_ref, dk_sum, dv_sum
):
    group = pl.program_id(1)
    width = q_ref.shape[1]
    key_rows = group_columns(k_ref[...], group, groups)
    value_rows = group_columns(v_ref[...], group, groups)
    cosine, sine = cos_ref[...], sin_ref[...]
    dk_sum[...] = jnp.zeros_like(dk_sum)
    dv_sum[...] = jnp.zeros_like(dv_sum)
    for start in range(0, SEQ, QUERY_TILE):
        keys = start + QUERY_TILE
        bias, _ = tile_bias(row_ref, col_ref, start, QUERY_TILE, keys)
        grad_queries = []
        for head in range(width // HD):
            columns = slice(head * HD, (head + 1) * HD)
            query_tile = q_ref[start:keys, columns]
            grad_tile = grad_ref[start:keys, columns]
            probs = tile_probs(key_rows[:keys], query_tile, bias)
            grad_probs = contract_cols(value_rows[:keys], grad_tile)
            delta = jnp.sum(probs * grad_probs, axis=0, keepdims=True)
            grad_scores = (probs * (grad_probs - delta)).astype(jnp.bfloat16)
            dv_sum[:keys, :] += matmul(probs.astype(jnp.bfloat16), grad_tile)
            dk_sum[:keys, :] += matmul(grad_scores, query_tile)
            grad_queries.append(contract_rows(key_rows[:keys], grad_scores))
        turned = jnp.concatenate(grad_queries, axis=0).T * HD ** (-0.5)
        dq_ref[start:keys, :] = unrotate(
            turned, cosine[start:keys], sine[start:keys]
        ).astype(jnp.bfloat16)
    for own in range(groups):

        @pl.when(group == own)
        def _():
            columns = slice(own * HD, (own + 1) * HD)
            dk_ref[:, columns] = dk_sum[...] * HD ** (-0.5)
            dv_ref[:, columns] = dv_sum[...].astype(jnp.bfloat16)

    @pl.when(group == groups - 1)
    def _():
        narrow = dk_ref.shape[1]
        dk_ref[...] = unrotate(dk_ref[...], cosine[:, :narrow], sine[:, :narrow])


def attention_specs(rows, heads_width, keys_width):
    groups = keys_width // HD
    width = heads_width // groups
    grid = (rows // SEQ, groups)
    wide = pl.BlockSpec((SEQ, width), lambda s, g: (s, g))
    narrow = pl.BlockSpec((SEQ, keys_width), lambda s, g: (s, 0))
    docs = [
        pl.BlockSpec((1, 1, SEQ), lambda s, g: (s, 0, 0)),
        pl.BlockSpec((SEQ, 1), lambda s, g: (s, 0)),
    ]
    tables = [pl.BlockSpec((SEQ, width), lambda s, g: (0, 0))] * 2
    return groups, grid, wide, narrow, docs, tables


def attention_cost(rows, heads_width, matmuls):
    pairs = rows * SEQ * (heads_width // HD)
    return pl.CostEstimate(
        flops=2 * matmuls * pairs * HD, transcendentals=pairs, bytes_accessed=16 * rows * heads_width
    )


def attend(query_pre, key_pre, value_pre, doc_row, doc_col, tables):
    rows, heads_width = query_pre.shape
    keys_width = key_pre.shape[1]
    groups, grid, wide, narrow, docs, table_specs = attention_specs(rows, heads_width, keys_width)
    bf = jnp.bfloat16
    return pl.pallas_call(
        functools.partial(attend_kernel, groups),
        name="attend",
        grid=grid,
        in_specs=[wide, narrow, narrow] + docs + table_specs,
        out_specs=[wide, narrow, narrow, wide],
        out_shape=[
            jax.ShapeDtypeStruct((rows, heads_width), bf),
            jax.ShapeDtypeStruct((rows, keys_width), bf),
            jax.ShapeDtypeStruct((rows, keys_width), bf),
            jax.ShapeDtypeStruct((rows, heads_width), bf),
        ],
        cost_estimate=attention_cost(rows, heads_width, 2),
    )(query_pre, key_pre, value_pre, doc_row, doc_col, *tables)


def attend_back(query_rows, key_rows, value_rows, grad_mixed, doc_row, doc_col, tables):
    rows, heads_width = query_rows.shape
    keys_width = key_rows.shape[1]
    groups, grid, wide, narrow, docs, table_specs = attention_specs(rows, heads_width, keys_width)
    bf = jnp.bfloat16
    return pl.pallas_call(
        functools.partial(attend_back_kernel, groups),
        name="attend_back",
        grid=grid,
        in_specs=[wide, narrow, narrow, wide] + docs + table_specs,
        out_specs=[wide, narrow, narrow],
        out_shape=[
            jax.ShapeDtypeStruct((rows, heads_width), bf),
            jax.ShapeDtypeStruct((rows, keys_width), jnp.float32),
            jax.ShapeDtypeStruct((rows, keys_width), bf),
        ],
        scratch_shapes=[pltpu.VMEM((SEQ, HD), jnp.float32)] * 2,
        cost_estimate=attention_cost(rows, heads_width, 5),
    )(query_rows, key_rows, value_rows, grad_mixed, doc_row, doc_col, *tables)


def swap(array, axis, size, bit):
    return lax.ppermute(array, axis, [(i, i ^ bit) for i in range(size)])


def gather_rows(own, size):
    if size != 4:
        return lax.all_gather(own, "tensor", axis=0, tiled=True)
    me = lax.axis_index("tensor")
    rows = own.shape[0]
    half = rows // 2
    near_x = swap(own, "tensor", size, 1)
    near_y = swap(own, "tensor", size, 2)
    far_low = swap(near_x[:half], "tensor", size, 2)
    far_high = swap(near_y[half:], "tensor", size, 1)
    whole = jnp.zeros((size * rows,) + own.shape[1:], own.dtype)
    far = (me ^ 3) * rows
    for piece, at in (
        (own, me * rows),
        (near_x, (me ^ 1) * rows),
        (near_y, (me ^ 2) * rows),
        (far_low, far),
        (far_high, far + half),
    ):
        whole = lax.dynamic_update_slice_in_dim(whole, piece, at, 0)
    return whole


def sum_rows(partial, size, beside=None):
    partial = partial.astype(jnp.bfloat16)
    if size != 4:
        return lax.psum_scatter(
            partial, "tensor", scatter_dimension=0, tiled=True
        ).astype(jnp.float32)
    me = lax.axis_index("tensor")
    rows = partial.shape[0] // size
    half = rows // 2

    def part(index, start=0, count=rows):
        return lax.dynamic_slice_in_dim(partial, index * rows + start, count, 0)

    from_x = swap(part(me ^ 3, 0, half), "tensor", size, 1)
    from_y = swap(part(me ^ 3, half, half), "tensor", size, 2)
    wide = jnp.float32
    to_y = jnp.concatenate(
        [
            (part(me ^ 2, 0, half).astype(wide) + from_x.astype(wide)).astype(jnp.bfloat16),
            part(me ^ 2, half, half),
        ]
    )
    to_x = jnp.concatenate(
        [
            part(me ^ 1, 0, half),
            (part(me ^ 1, half, half).astype(wide) + from_y.astype(wide)).astype(jnp.bfloat16),
        ]
    )
    last_y = swap(to_y, "tensor", size, 2)
    last_x = swap(to_x, "tensor", size, 1)
    own = part(me)
    if beside is not None:
        own, _ = lax.optimization_barrier((own, beside))
    return own.astype(wide) + last_x.astype(wide) + last_y.astype(wide)


def sum_all(array, axis, size):
    if size & (size - 1):
        return lax.psum(array, axis)
    bit = 1
    while bit < size:
        array = array + swap(array, axis, size, bit)
        bit *= 2
    return array


def parity_columns(rows, size):
    mine = lax.axis_index("dp") % 2
    cut = rows.reshape(rows.shape[0], size // 2, 2, rows.shape[1] // size)

    def pick(which):
        return lax.dynamic_index_in_dim(cut, which, 2, keepdims=False).reshape(rows.shape[0], -1)

    return pick(mine), pick(1 - mine)


def pair_grad(parities, right_side, size):
    mine, other = parities
    from_pair = swap(contract_rows(other, right_side).astype(jnp.bfloat16), "dp", size, 1)
    pair_sum = contract_rows(mine, right_side) + from_pair.astype(jnp.float32)
    return pair_sum.astype(jnp.bfloat16)


def sum_pairs(pair_sum, size):
    groups = [list(range(0, size, 2)), list(range(1, size, 2))]
    return lax.psum_scatter(
        pair_sum,
        "dp",
        scatter_dimension=0,
        tiled=True,
        axis_index_groups=groups,
    ).astype(jnp.float32)


def per_device(
    dp,
    tp,
    block_input,
    attn_gain,
    w_query,
    w_key,
    w_value,
    w_out,
    mlp_gain,
    w_gate,
    w_up,
    w_down,
    doc_ids,
    cotangent,
):
    heads_width, keys_width = w_query.shape[1], w_key.shape[1]
    splits = (heads_width, heads_width + keys_width)

    def gather(weight):
        return lax.all_gather(weight, "dp", axis=0, tiled=True)

    narrow = splits[1] + keys_width
    small_full = gather(jnp.concatenate([w_query, w_key, w_value, w_out], axis=1))
    qkv_full, out_full = small_full[:, :narrow], small_full[:, narrow:]
    gate_up_full = gather(jnp.concatenate([w_gate, w_up], axis=1))
    gate_full, up_full = jnp.split(gate_up_full, 2, axis=1)
    down_full = gather(w_down)

    live_all = (doc_ids >= 0).astype(jnp.float32)
    doc_row = doc_ids.reshape(-1, 1, SEQ)
    doc_col = doc_ids.reshape(-1, 1)
    tables = rotary_tables(SEQ, HD, heads_width // keys_width)

    input_own = block_input.astype(jnp.float32)
    scale_one = norm_scale(input_own)
    normed_one = gather_rows(
        (input_own * scale_one * attn_gain[None, :]).astype(jnp.bfloat16), tp
    )
    grad_full = gather_rows(cotangent, tp)

    qkv_pre = matmul(normed_one, qkv_full)
    query_rows, key_rows, value_rows, mixed_all = attend(
        *jnp.split(qkv_pre, splits, axis=1), doc_row, doc_col, tables
    )
    residual_own = input_own + sum_rows(contract_cols(mixed_all, out_full), tp)
    scale_two_own = norm_scale(residual_own)
    normed_two = gather_rows(
        (residual_own * scale_two_own * mlp_gain[None, :]).astype(jnp.bfloat16), tp
    )
    gate_pre = matmul(normed_two, gate_full)
    up_pre = matmul(normed_two, up_full)
    sigmoid_gate = jax.nn.sigmoid(gate_pre)
    silu_gate = gate_pre * sigmoid_gate
    hidden = (silu_gate * up_pre).astype(jnp.bfloat16)
    pair_down = pair_grad(parity_columns(grad_full, dp), hidden, dp)
    one_parities = parity_columns(normed_one, dp)
    two_parities = parity_columns(normed_two, dp)
    pair_down, down_full, one_parities, two_parities = lax.optimization_barrier(
        (pair_down, down_full, one_parities, two_parities)
    )
    grad_down = sum_pairs(pair_down, dp)

    grad_hidden = matmul(grad_full, down_full)
    grad_gate_pre = (
        grad_hidden * up_pre * sigmoid_gate * (1.0 + gate_pre * (1.0 - sigmoid_gate))
    ).astype(jnp.bfloat16)
    grad_up_pre = (grad_hidden * silu_gate).astype(jnp.bfloat16)
    grad_gate_up = jnp.concatenate(
        lax.optimization_barrier((grad_gate_pre, grad_up_pre)), axis=1
    )
    grad_normed_part = contract_cols(grad_gate_up, gate_up_full).astype(jnp.bfloat16)
    grad_normed_part, grad_gate_up = lax.optimization_barrier((grad_normed_part, grad_gate_up))
    pair_gate_up = pair_grad(two_parities, grad_gate_up, dp)
    grad_normed_own = sum_rows(grad_normed_part, tp, beside=pair_gate_up)
    grad_normed_own, pair_gate_up = lax.optimization_barrier((grad_normed_own, pair_gate_up))
    grad_gate, grad_up = jnp.split(sum_pairs(pair_gate_up, dp), 2, axis=1)
    grad_mlp_gain = jnp.sum(grad_normed_own * residual_own * scale_two_own, axis=0)
    grad_residual_own = cotangent.astype(jnp.float32) + norm_back(
        grad_normed_own, residual_own, scale_two_own, mlp_gain
    )
    to_gather, hidden = lax.optimization_barrier(
        (grad_residual_own.astype(jnp.bfloat16), hidden)
    )
    grad_residual_bf = gather_rows(to_gather, tp)
    block_part = contract_cols(hidden, down_full).astype(jnp.bfloat16)
    grad_residual_bf, block_part = lax.optimization_barrier((grad_residual_bf, block_part))
    grad_mixed = (matmul(grad_residual_bf, out_full) * live_all[:, None]).astype(jnp.bfloat16)
    block_output = (residual_own + sum_rows(block_part, tp)).astype(jnp.bfloat16)
    grad_query_rows, grad_keys, grad_value_rows = attend_back(
        query_rows, key_rows, value_rows, grad_mixed, doc_row, doc_col, tables
    )
    grad_qkv_rows = jnp.concatenate(
        [grad_query_rows, grad_keys.astype(jnp.bfloat16), grad_value_rows], axis=1
    )
    grad_one_part = contract_cols(grad_qkv_rows, qkv_full).astype(jnp.bfloat16)
    grad_one_part, grad_qkv_rows, mixed_all, grad_residual_bf = lax.optimization_barrier(
        (grad_one_part, grad_qkv_rows, mixed_all, grad_residual_bf)
    )
    pair_small = jnp.concatenate(
        [
            pair_grad(one_parities, grad_qkv_rows, dp),
            pair_grad(parity_columns(grad_residual_bf, dp), mixed_all, dp),
        ],
        axis=1,
    )
    grad_query, grad_key, grad_value, grad_out = jnp.split(
        sum_pairs(pair_small, dp), splits + (narrow,), axis=1
    )
    grad_normed_one = sum_rows(grad_one_part, tp)
    grad_attn_gain = jnp.sum(grad_normed_one * input_own * scale_one, axis=0)
    input_grad = (
        grad_residual_own + norm_back(grad_normed_one, input_own, scale_one, attn_gain)
    ).astype(jnp.bfloat16)
    gains = jnp.stack([grad_attn_gain, grad_mlp_gain])
    gains = sum_all(sum_all(gains, "tensor", tp), "dp", dp)
    return (
        block_output,
        input_grad,
        grad_query,
        grad_key,
        grad_value,
        grad_out,
        grad_gate,
        grad_up,
        grad_down,
        gains[0],
        gains[1],
    )


def solution(mesh):
    in_specs = (
        P(("dp", "tensor"), None),
        P(),
        P("dp", "tensor"),
        P("dp", "tensor"),
        P("dp", "tensor"),
        P("dp", "tensor"),
        P(),
        P("dp", "tensor"),
        P("dp", "tensor"),
        P("dp", "tensor"),
        P("dp"),
        P(("dp", "tensor"), None),
    )
    out_specs = (
        P(("dp", "tensor"), None),
        P(("dp", "tensor"), None),
        P("dp", "tensor"),
        P("dp", "tensor"),
        P("dp", "tensor"),
        P("dp", "tensor"),
        P("dp", "tensor"),
        P("dp", "tensor"),
        P("dp", "tensor"),
        P(),
        P(),
    )
    return jax.shard_map(
        functools.partial(per_device, mesh.shape["dp"], mesh.shape["tensor"]),
        mesh=mesh,
        in_specs=in_specs,
        out_specs=out_specs,
        check_vma=False,
    )
```

```python
import functools

import jax
import jax.numpy as jnp
from jax import lax
from jax.experimental import pallas as pl
from jax.experimental.pallas import tpu as pltpu
from jax.sharding import PartitionSpec as P


HD = 64
SEQ = 512
QUERY_TILE = 256

EPSILON = 1e-05
ROPE_BASE = 500000.0
NEG_LARGE = -1e30


def rotary_tables(length, head_dim, copies):
    half_dim = head_dim // 2
    frequency = ROPE_BASE ** (-(jnp.arange(half_dim, dtype=jnp.float32) * (2.0 / head_dim)))
    angles = jnp.arange(length, dtype=jnp.float32)[:, None] * frequency[None, :]
    angles = jnp.concatenate([angles, angles] * copies, axis=1)
    return (jnp.cos(angles), jnp.sin(angles))


def norm_scale(tensor_rows):
    return lax.rsqrt(jnp.mean(tensor_rows * tensor_rows, axis=1, keepdims=True) + EPSILON)


def norm_back(grad_normed, tensor_rows, row_scale, gain_row):
    weighted = grad_normed * gain_row[None, :]
    inner_mean = jnp.mean(weighted * tensor_rows, axis=1, keepdims=True)
    return row_scale * weighted - tensor_rows * (row_scale * row_scale * row_scale) * inner_mean


def contract_rows(left_side, right_side):
    return lax.dot_general(
        left_side, right_side, (((0,), (0,)), ((), ())), preferred_element_type=jnp.float32
    )


def contract_cols(left_side, right_side):
    return lax.dot_general(
        left_side, right_side, (((1,), (1,)), ((), ())), preferred_element_type=jnp.float32
    )


def matmul(left_side, right_side):
    return jnp.dot(left_side, right_side, preferred_element_type=jnp.float32)


def half_turn(rows):
    width = rows.shape[1]
    first = lax.broadcasted_iota(jnp.int32, rows.shape, 1) % HD < HD // 2
    if width % 128 == 0:
        later = pltpu.roll(rows, width - HD // 2, axis=1)
        before = pltpu.roll(rows, HD // 2, axis=1)
        return jnp.where(first, later, before), first
    halves = [rows[:, at : at + HD // 2] for at in range(0, width, HD // 2)]
    swapped = [halves[i ^ 1] for i in range(len(halves))]
    return jnp.concatenate(swapped, axis=1), first


def rotate(rows, cosine, sine):
    turned, first = half_turn(rows)
    return rows * cosine + jnp.where(first, -turned, turned) * sine


def unrotate(rows, cosine, sine):
    turned, first = half_turn(rows * sine)
    return rows * cosine + jnp.where(first, turned, -turned)


def group_columns(rows, group, groups):
    picked = rows[:, :HD]
    for other in range(1, groups):
        picked = jnp.where(group == other, rows[:, other * HD : (other + 1) * HD], picked)
    return picked


def tile_bias(doc_row, doc_col, start, tile, keys):
    query_doc = doc_row[0, :, start : start + tile]
    key_doc = doc_col[:keys, :]
    key_at = lax.broadcasted_iota(jnp.int32, (keys, tile), 0)
    query_at = lax.broadcasted_iota(jnp.int32, (keys, tile), 1) + start
    same = (query_doc == key_doc) & (key_doc >= 0) & (key_at <= query_at)
    live = (query_doc >= 0).astype(jnp.float32)
    return jnp.where(same | (key_at == query_at), 0.0, NEG_LARGE), live


def tile_probs(keys_rows, query_tile, bias):
    scores = contract_cols(keys_rows, query_tile) * HD ** (-0.5) + bias
    weights = jnp.exp(scores - jnp.max(scores, axis=0, keepdims=True))
    return weights * (1.0 / jnp.sum(weights, axis=0, keepdims=True))


def attend_kernel(
    groups, q_ref, k_ref, v_ref, row_ref, col_ref, cos_ref, sin_ref,
    q_out, k_out, v_out, mixed_ref
):
    group = pl.program_id(1)
    width = q_ref.shape[1]
    narrow = k_ref.shape[1]
    query_rows = rotate(q_ref[...], cos_ref[...], sin_ref[...]).astype(jnp.bfloat16)
    key_all = rotate(k_ref[...], cos_ref[:, :narrow], sin_ref[:, :narrow]).astype(jnp.bfloat16)
    value_all = v_ref[...].astype(jnp.bfloat16)
    q_out[...] = query_rows
    k_out[...] = key_all
    v_out[...] = value_all
    key_rows = group_columns(key_all, group, groups)
    value_rows = group_columns(value_all, group, groups)
    for start in range(0, SEQ, QUERY_TILE):
        keys = start + QUERY_TILE
        bias, live = tile_bias(row_ref, col_ref, start, QUERY_TILE, keys)
        mixed = []
        for head in range(width // HD):
            query_tile = query_rows[start:keys, head * HD : (head + 1) * HD]
            probs = tile_probs(key_rows[:keys], query_tile, bias).astype(jnp.bfloat16)
            mixed.append(contract_rows(value_rows[:keys], probs) * live)
        mixed_ref[start:keys, :] = jnp.concatenate(mixed, axis=0).T.astype(jnp.bfloat16)


def attend_back_kernel(
    groups, q_ref, k_ref, v_ref, grad_ref, row_ref, col_ref, cos_ref, sin_ref,
    dq_ref, dk_ref, dv_ref, dk_sum, dv_sum
):
    group = pl.program_id(1)
    width = q_ref.shape[1]
    key_rows = group_columns(k_ref[...], group, groups)
    value_rows = group_columns(v_ref[...], group, groups)
    cosine, sine = cos_ref[...], sin_ref[...]
    dk_sum[...] = jnp.zeros_like(dk_sum)
    dv_sum[...] = jnp.zeros_like(dv_sum)
    for start in range(0, SEQ, QUERY_TILE):
        keys = start + QUERY_TILE
        bias, _ = tile_bias(row_ref, col_ref, start, QUERY_TILE, keys)
        grad_queries = []
        for head in range(width // HD):
            columns = slice(head * HD, (head + 1) * HD)
            query_tile = q_ref[start:keys, columns]
            grad_tile = grad_ref[start:keys, columns]
            probs = tile_probs(key_rows[:keys], query_tile, bias)
            grad_probs = contract_cols(value_rows[:keys], grad_tile)
            delta = jnp.sum(probs * grad_probs, axis=0, keepdims=True)
            grad_scores = (probs * (grad_probs - delta)).astype(jnp.bfloat16)
            dv_sum[:keys, :] += matmul(probs.astype(jnp.bfloat16), grad_tile)
            dk_sum[:keys, :] += matmul(grad_scores, query_tile)
            grad_queries.append(contract_rows(key_rows[:keys], grad_scores))
        turned = jnp.concatenate(grad_queries, axis=0).T * HD ** (-0.5)
        dq_ref[start:keys, :] = unrotate(
            turned, cosine[start:keys], sine[start:keys]
        ).astype(jnp.bfloat16)
    for own in range(groups):

        @pl.when(group == own)
        def _():
            columns = slice(own * HD, (own + 1) * HD)
            dk_ref[:, columns] = dk_sum[...] * HD ** (-0.5)
            dv_ref[:, columns] = dv_sum[...].astype(jnp.bfloat16)

    @pl.when(group == groups - 1)
    def _():
        narrow = dk_ref.shape[1]
        dk_ref[...] = unrotate(dk_ref[...], cosine[:, :narrow], sine[:, :narrow])


def attention_specs(rows, heads_width, keys_width):
    groups = keys_width // HD
    width = heads_width // groups
    grid = (rows // SEQ, groups)
    wide = pl.BlockSpec((SEQ, width), lambda s, g: (s, g))
    narrow = pl.BlockSpec((SEQ, keys_width), lambda s, g: (s, 0))
    docs = [
        pl.BlockSpec((1, 1, SEQ), lambda s, g: (s, 0, 0)),
        pl.BlockSpec((SEQ, 1), lambda s, g: (s, 0)),
    ]
    tables = [pl.BlockSpec((SEQ, width), lambda s, g: (0, 0))] * 2
    return groups, grid, wide, narrow, docs, tables


def attention_cost(rows, heads_width, matmuls):
    pairs = rows * SEQ * (heads_width // HD)
    return pl.CostEstimate(
        flops=2 * matmuls * pairs * HD, transcendentals=pairs, bytes_accessed=16 * rows * heads_width
    )


def attend(query_pre, key_pre, value_pre, doc_row, doc_col, tables):
    rows, heads_width = query_pre.shape
    keys_width = key_pre.shape[1]
    groups, grid, wide, narrow, docs, table_specs = attention_specs(rows, heads_width, keys_width)
    bf = jnp.bfloat16
    return pl.pallas_call(
        functools.partial(attend_kernel, groups),
        name="attend",
        grid=grid,
        in_specs=[wide, narrow, narrow] + docs + table_specs,
        out_specs=[wide, narrow, narrow, wide],
        out_shape=[
            jax.ShapeDtypeStruct((rows, heads_width), bf),
            jax.ShapeDtypeStruct((rows, keys_width), bf),
            jax.ShapeDtypeStruct((rows, keys_width), bf),
            jax.ShapeDtypeStruct((rows, heads_width), bf),
        ],
        cost_estimate=attention_cost(rows, heads_width, 2),
    )(query_pre, key_pre, value_pre, doc_row, doc_col, *tables)


def attend_back(query_rows, key_rows, value_rows, grad_mixed, doc_row, doc_col, tables):
    rows, heads_width = query_rows.shape
    keys_width = key_rows.shape[1]
    groups, grid, wide, narrow, docs, table_specs = attention_specs(rows, heads_width, keys_width)
    bf = jnp.bfloat16
    return pl.pallas_call(
        functools.partial(attend_back_kernel, groups),
        name="attend_back",
        grid=grid,
        in_specs=[wide, narrow, narrow, wide] + docs + table_specs,
        out_specs=[wide, narrow, narrow],
        out_shape=[
            jax.ShapeDtypeStruct((rows, heads_width), bf),
            jax.ShapeDtypeStruct((rows, keys_width), jnp.float32),
            jax.ShapeDtypeStruct((rows, keys_width), bf),
        ],
        scratch_shapes=[pltpu.VMEM((SEQ, HD), jnp.float32)] * 2,
        cost_estimate=attention_cost(rows, heads_width, 5),
    )(query_rows, key_rows, value_rows, grad_mixed, doc_row, doc_col, *tables)


def swap(array, axis, size, bit):
    return lax.ppermute(array, axis, [(i, i ^ bit) for i in range(size)])


def gather_rows(own, size):
    if size != 4:
        return lax.all_gather(own, "tensor", axis=0, tiled=True)
    me = lax.axis_index("tensor")
    rows = own.shape[0]
    half = rows // 2
    near_x = swap(own, "tensor", size, 1)
    near_y = swap(own, "tensor", size, 2)
    far_low = swap(near_x[:half], "tensor", size, 2)
    far_high = swap(near_y[half:], "tensor", size, 1)
    whole = jnp.zeros((size * rows,) + own.shape[1:], own.dtype)
    far = (me ^ 3) * rows
    for piece, at in (
        (own, me * rows),
        (near_x, (me ^ 1) * rows),
        (near_y, (me ^ 2) * rows),
        (far_low, far),
        (far_high, far + half),
    ):
        whole = lax.dynamic_update_slice_in_dim(whole, piece, at, 0)
    return whole


def sum_rows(partial, size, beside=None):
    partial = partial.astype(jnp.bfloat16)
    if size != 4:
        return lax.psum_scatter(
            partial, "tensor", scatter_dimension=0, tiled=True
        ).astype(jnp.float32)
    me = lax.axis_index("tensor")
    rows = partial.shape[0] // size
    half = rows // 2

    def part(index, start=0, count=rows):
        return lax.dynamic_slice_in_dim(partial, index * rows + start, count, 0)

    from_x = swap(part(me ^ 3, 0, half), "tensor", size, 1)
    from_y = swap(part(me ^ 3, half, half), "tensor", size, 2)
    wide = jnp.float32
    near_low, near_high = part(me ^ 2, 0, half), part(me ^ 1, half, half)
    if beside is not None:
        near_low, near_high, _ = lax.optimization_barrier((near_low, near_high, beside))
    near_low = (near_low.astype(wide) + from_x.astype(wide)).astype(jnp.bfloat16)
    near_high = (near_high.astype(wide) + from_y.astype(wide)).astype(jnp.bfloat16)
    to_y = jnp.concatenate([near_low, part(me ^ 2, half, half)])
    to_x = jnp.concatenate([part(me ^ 1, 0, half), near_high])
    last_y = swap(to_y, "tensor", size, 2)
    last_x = swap(to_x, "tensor", size, 1)
    return part(me).astype(wide) + last_x.astype(wide) + last_y.astype(wide)


def sum_all(array, axis, size):
    if size & (size - 1):
        return lax.psum(array, axis)
    bit = 1
    while bit < size:
        array = array + swap(array, axis, size, bit)
        bit *= 2
    return array


def odd_device():
    return lax.axis_index("dp") % 2 == 1


def to_pairs(rows, size):
    cut = rows.reshape(rows.shape[0], size // 2, 2, rows.shape[1] // size)
    even = cut[:, :, 0].reshape(rows.shape[0], -1)
    odd = cut[:, :, 1].reshape(rows.shape[0], -1)
    flip = odd_device()
    return jnp.concatenate([jnp.where(flip, odd, even), jnp.where(flip, even, odd)], axis=1)


def from_pairs(rows, size):
    mine, other = jnp.split(rows, 2, axis=1)
    flip = odd_device()
    shape = (rows.shape[0], size // 2, rows.shape[1] // size)
    even = jnp.where(flip, other, mine).reshape(shape)
    odd = jnp.where(flip, mine, other).reshape(shape)
    return jnp.stack([even, odd], axis=2).reshape(rows.shape)


def parity_groups(size):
    return [list(range(0, size, 2)), list(range(1, size, 2))]


def gather_parity(weight, size):
    return lax.all_gather(
        weight, "dp", axis=0, tiled=True, axis_index_groups=parity_groups(size)
    )


def with_partner(mine, size):
    return mine, swap(mine, "dp", size, 1)


def columns(pair, start, stop):
    return tuple(part[:, start:stop] for part in pair)


def matmul_pair(left_side, pair):
    mine, other = jnp.split(left_side, 2, axis=1)
    return matmul(other, pair[1]) + matmul(mine, pair[0])


def contract_pair(left_side, pair):
    return jnp.concatenate(
        [contract_cols(left_side, part).astype(jnp.bfloat16) for part in pair], axis=1
    )


def other_grad(left_side, right_side):
    return contract_rows(jnp.split(left_side, 2, axis=1)[1], right_side).astype(jnp.bfloat16)


def pair_grad(left_side, right_side, size, other=None):
    other = other_grad(left_side, right_side) if other is None else other
    from_pair = swap(other, "dp", size, 1)
    pair_sum = contract_rows(jnp.split(left_side, 2, axis=1)[0], right_side) + from_pair.astype(jnp.float32)
    return pair_sum.astype(jnp.bfloat16)


def sum_pairs(pair_sum, size):
    return lax.psum_scatter(
        pair_sum,
        "dp",
        scatter_dimension=0,
        tiled=True,
        axis_index_groups=parity_groups(size),
    ).astype(jnp.float32)


def per_device(
    dp,
    tp,
    block_input,
    attn_gain,
    w_query,
    w_key,
    w_value,
    w_out,
    mlp_gain,
    w_gate,
    w_up,
    w_down,
    doc_ids,
    cotangent,
):
    heads_width, keys_width = w_query.shape[1], w_key.shape[1]
    splits = (heads_width, heads_width + keys_width)

    narrow = splits[1] + keys_width
    small_full = with_partner(
        gather_parity(jnp.concatenate([w_query, w_key, w_value, w_out], axis=1), dp), dp
    )
    qkv_full = columns(small_full, 0, narrow)
    out_full = columns(small_full, narrow, narrow + heads_width)
    gate_up_mine = gather_parity(jnp.concatenate([w_gate, w_up], axis=1), dp)
    down_mine = gather_parity(w_down, dp)
    attn_gain = to_pairs(attn_gain[None, :], dp)[0]
    mlp_gain = to_pairs(mlp_gain[None, :], dp)[0]
    cotangent = to_pairs(cotangent, dp)

    live_all = (doc_ids >= 0).astype(jnp.float32)
    doc_row = doc_ids.reshape(-1, 1, SEQ)
    doc_col = doc_ids.reshape(-1, 1)
    tables = rotary_tables(SEQ, HD, heads_width // keys_width)

    input_own = to_pairs(block_input, dp).astype(jnp.float32)
    scale_one = norm_scale(input_own)
    normed_one = gather_rows(
        (input_own * scale_one * attn_gain[None, :]).astype(jnp.bfloat16), tp
    )
    grad_full = gather_rows(cotangent, tp)

    qkv_pre = matmul_pair(normed_one, qkv_full)
    query_rows, key_rows, value_rows, mixed_all = attend(
        *jnp.split(qkv_pre, splits, axis=1), doc_row, doc_col, tables
    )
    residual_own = input_own + sum_rows(contract_pair(mixed_all, out_full), tp)
    scale_two_own = norm_scale(residual_own)
    normed_two = gather_rows(
        (residual_own * scale_two_own * mlp_gain[None, :]).astype(jnp.bfloat16), tp
    )
    normed_two, gate_up_mine = lax.optimization_barrier((normed_two, gate_up_mine))
    gate_up_full = with_partner(gate_up_mine, dp)
    units = w_gate.shape[1]
    gate_full = columns(gate_up_full, 0, units)
    up_full = columns(gate_up_full, units, 2 * units)
    gate_pre = matmul_pair(normed_two, gate_full)
    up_pre = matmul_pair(normed_two, up_full)
    sigmoid_gate = jax.nn.sigmoid(gate_pre)
    silu_gate = gate_pre * sigmoid_gate
    hidden = (silu_gate * up_pre).astype(jnp.bfloat16)
    pair_down = pair_grad(grad_full, hidden, dp)
    pair_down, down_mine = lax.optimization_barrier((pair_down, down_mine))
    down_full = with_partner(down_mine, dp)
    grad_down = sum_pairs(pair_down, dp)

    grad_hidden = matmul_pair(grad_full, down_full)
    grad_gate_pre = (
        grad_hidden * up_pre * sigmoid_gate * (1.0 + gate_pre * (1.0 - sigmoid_gate))
    ).astype(jnp.bfloat16)
    grad_up_pre = (grad_hidden * silu_gate).astype(jnp.bfloat16)
    grad_gate_up = jnp.concatenate(
        lax.optimization_barrier((grad_gate_pre, grad_up_pre)), axis=1
    )
    other_gate_up = other_grad(normed_two, grad_gate_up)
    other_gate_up, grad_gate_up = lax.optimization_barrier((other_gate_up, grad_gate_up))
    grad_normed_part = contract_pair(grad_gate_up, gate_up_full)
    grad_normed_part, grad_gate_up = lax.optimization_barrier((grad_normed_part, grad_gate_up))
    pair_gate_up = pair_grad(normed_two, grad_gate_up, dp, other_gate_up)
    grad_normed_own = sum_rows(grad_normed_part, tp, beside=pair_gate_up)
    grad_gate, grad_up = jnp.split(sum_pairs(pair_gate_up, dp), 2, axis=1)
    grad_mlp_gain = jnp.sum(grad_normed_own * residual_own * scale_two_own, axis=0)
    grad_residual_own = cotangent.astype(jnp.float32) + norm_back(
        grad_normed_own, residual_own, scale_two_own, mlp_gain
    )
    to_gather, hidden = lax.optimization_barrier(
        (grad_residual_own.astype(jnp.bfloat16), hidden)
    )
    grad_residual_bf = gather_rows(to_gather, tp)
    block_part = contract_pair(hidden, down_full)
    grad_residual_bf, block_part = lax.optimization_barrier((grad_residual_bf, block_part))
    grad_mixed = (matmul_pair(grad_residual_bf, out_full) * live_all[:, None]).astype(jnp.bfloat16)
    block_output = from_pairs(
        (residual_own + sum_rows(block_part, tp)).astype(jnp.bfloat16), dp
    )
    grad_query_rows, grad_keys, grad_value_rows = attend_back(
        query_rows, key_rows, value_rows, grad_mixed, doc_row, doc_col, tables
    )
    grad_qkv_rows = jnp.concatenate(
        [grad_query_rows, grad_keys.astype(jnp.bfloat16), grad_value_rows], axis=1
    )
    grad_one_part = contract_pair(grad_qkv_rows, qkv_full)
    grad_one_part, grad_qkv_rows, mixed_all, grad_residual_bf = lax.optimization_barrier(
        (grad_one_part, grad_qkv_rows, mixed_all, grad_residual_bf)
    )
    pair_small = jnp.concatenate(
        [
            pair_grad(normed_one, grad_qkv_rows, dp),
            pair_grad(grad_residual_bf, mixed_all, dp),
        ],
        axis=1,
    )
    grad_query, grad_key, grad_value, grad_out = jnp.split(
        sum_pairs(pair_small, dp), splits + (narrow,), axis=1
    )
    grad_normed_one = sum_rows(grad_one_part, tp)
    grad_attn_gain = jnp.sum(grad_normed_one * input_own * scale_one, axis=0)
    input_grad = from_pairs(
        (
            grad_residual_own + norm_back(grad_normed_one, input_own, scale_one, attn_gain)
        ).astype(jnp.bfloat16),
        dp,
    )
    gains = from_pairs(jnp.stack([grad_attn_gain, grad_mlp_gain]), dp)
    gains = sum_all(sum_all(gains, "tensor", tp), "dp", dp)
    return (
        block_output,
        input_grad,
        grad_query,
        grad_key,
        grad_value,
        grad_out,
        grad_gate,
        grad_up,
        grad_down,
        gains[0],
        gains[1],
    )


def solution(mesh):
    in_specs = (
        P(("dp", "tensor"), None),
        P(),
        P("dp", "tensor"),
        P("dp", "tensor"),
        P("dp", "tensor"),
        P("dp", "tensor"),
        P(),
        P("dp", "tensor"),
        P("dp", "tensor"),
        P("dp", "tensor"),
        P("dp"),
        P(("dp", "tensor"), None),
    )
    out_specs = (
        P(("dp", "tensor"), None),
        P(("dp", "tensor"), None),
        P("dp", "tensor"),
        P("dp", "tensor"),
        P("dp", "tensor"),
        P("dp", "tensor"),
        P("dp", "tensor"),
        P("dp", "tensor"),
        P("dp", "tensor"),
        P(),
        P(),
    )
    return jax.shard_map(
        functools.partial(per_device, mesh.shape["dp"], mesh.shape["tensor"]),
        mesh=mesh,
        in_specs=in_specs,
        out_specs=out_specs,
        check_vma=False,
    )
```

```python
import functools

import jax
import jax.numpy as jnp
from jax import lax
from jax.experimental import pallas as pl
from jax.experimental.pallas import tpu as pltpu
from jax.experimental.layout import Layout, with_layout_constraint
from jax.sharding import PartitionSpec as P


HD = 64
SEQ = 512
QUERY_TILE = 256

EPSILON = 1e-05
ROPE_BASE = 500000.0
NEG_LARGE = -1e30


def rotary_tables(length, head_dim, copies):
    half_dim = head_dim // 2
    frequency = ROPE_BASE ** (-(jnp.arange(half_dim, dtype=jnp.float32) * (2.0 / head_dim)))
    angles = jnp.arange(length, dtype=jnp.float32)[:, None] * frequency[None, :]
    angles = jnp.concatenate([angles, angles] * copies, axis=1)
    return (jnp.cos(angles), jnp.sin(angles))


def norm_scale(tensor_rows):
    return lax.rsqrt(jnp.mean(tensor_rows * tensor_rows, axis=1, keepdims=True) + EPSILON)


def norm_back(grad_normed, tensor_rows, row_scale, gain_row):
    weighted = grad_normed * gain_row[None, :]
    inner_mean = jnp.mean(weighted * tensor_rows, axis=1, keepdims=True)
    return row_scale * weighted - tensor_rows * (row_scale * row_scale * row_scale) * inner_mean


def contract_rows(left_side, right_side):
    return lax.dot_general(
        left_side, right_side, (((0,), (0,)), ((), ())), preferred_element_type=jnp.float32
    )


def contract_cols(left_side, right_side):
    return lax.dot_general(
        left_side, right_side, (((1,), (1,)), ((), ())), preferred_element_type=jnp.float32
    )


def matmul(left_side, right_side):
    return jnp.dot(left_side, right_side, preferred_element_type=jnp.float32)


def half_turn(rows):
    width = rows.shape[1]
    first = lax.broadcasted_iota(jnp.int32, rows.shape, 1) % HD < HD // 2
    if width % 128 == 0:
        later = pltpu.roll(rows, width - HD // 2, axis=1)
        before = pltpu.roll(rows, HD // 2, axis=1)
        return jnp.where(first, later, before), first
    halves = [rows[:, at : at + HD // 2] for at in range(0, width, HD // 2)]
    swapped = [halves[i ^ 1] for i in range(len(halves))]
    return jnp.concatenate(swapped, axis=1), first


def rotate(rows, cosine, sine):
    turned, first = half_turn(rows)
    return rows * cosine + jnp.where(first, -turned, turned) * sine


def unrotate(rows, cosine, sine):
    turned, first = half_turn(rows * sine)
    return rows * cosine + jnp.where(first, turned, -turned)


def group_columns(rows, group, groups):
    picked = rows[:, :HD]
    for other in range(1, groups):
        picked = jnp.where(group == other, rows[:, other * HD : (other + 1) * HD], picked)
    return picked


def tile_bias(doc_row, doc_col, start, tile, keys):
    query_doc = doc_row[0, :, start : start + tile]
    key_doc = doc_col[:keys, :]
    key_at = lax.broadcasted_iota(jnp.int32, (keys, tile), 0)
    query_at = lax.broadcasted_iota(jnp.int32, (keys, tile), 1) + start
    same = (query_doc == key_doc) & (key_doc >= 0) & (key_at <= query_at)
    live = (query_doc >= 0).astype(jnp.float32)
    return jnp.where(same | (key_at == query_at), 0.0, NEG_LARGE), live


def tile_probs(keys_rows, query_tile, bias):
    scores = contract_cols(keys_rows, query_tile) * HD ** (-0.5) + bias
    weights = jnp.exp(scores - jnp.max(scores, axis=0, keepdims=True))
    return weights * (1.0 / jnp.sum(weights, axis=0, keepdims=True))


def attend_kernel(
    groups, q_ref, k_ref, v_ref, row_ref, col_ref, cos_ref, sin_ref,
    q_out, k_out, v_out, mixed_ref
):
    group = pl.program_id(1)
    width = q_ref.shape[1]
    narrow = k_ref.shape[1]
    query_rows = rotate(q_ref[...], cos_ref[...], sin_ref[...]).astype(jnp.bfloat16)
    key_all = rotate(k_ref[...], cos_ref[:, :narrow], sin_ref[:, :narrow]).astype(jnp.bfloat16)
    value_all = v_ref[...].astype(jnp.bfloat16)
    q_out[...] = query_rows
    k_out[...] = key_all
    v_out[...] = value_all
    key_rows = group_columns(key_all, group, groups)
    value_rows = group_columns(value_all, group, groups)
    for start in range(0, SEQ, QUERY_TILE):
        keys = start + QUERY_TILE
        bias, live = tile_bias(row_ref, col_ref, start, QUERY_TILE, keys)
        mixed = []
        for head in range(width // HD):
            query_tile = query_rows[start:keys, head * HD : (head + 1) * HD]
            probs = tile_probs(key_rows[:keys], query_tile, bias).astype(jnp.bfloat16)
            mixed.append(contract_rows(value_rows[:keys], probs) * live)
        mixed_ref[start:keys, :] = jnp.concatenate(mixed, axis=0).T.astype(jnp.bfloat16)


def attend_back_kernel(
    groups, q_ref, k_ref, v_ref, grad_ref, row_ref, col_ref, cos_ref, sin_ref,
    dq_ref, dk_ref, dv_ref, dk_sum, dv_sum
):
    group = pl.program_id(1)
    width = q_ref.shape[1]
    key_rows = group_columns(k_ref[...], group, groups)
    value_rows = group_columns(v_ref[...], group, groups)
    cosine, sine = cos_ref[...], sin_ref[...]
    dk_sum[...] = jnp.zeros_like(dk_sum)
    dv_sum[...] = jnp.zeros_like(dv_sum)
    for start in range(0, SEQ, QUERY_TILE):
        keys = start + QUERY_TILE
        bias, _ = tile_bias(row_ref, col_ref, start, QUERY_TILE, keys)
        grad_queries = []
        for head in range(width // HD):
            columns = slice(head * HD, (head + 1) * HD)
            query_tile = q_ref[start:keys, columns]
            grad_tile = grad_ref[start:keys, columns]
            probs = tile_probs(key_rows[:keys], query_tile, bias)
            grad_probs = contract_cols(value_rows[:keys], grad_tile)
            delta = jnp.sum(probs * grad_probs, axis=0, keepdims=True)
            grad_scores = (probs * (grad_probs - delta)).astype(jnp.bfloat16)
            dv_sum[:keys, :] += matmul(probs.astype(jnp.bfloat16), grad_tile)
            dk_sum[:keys, :] += matmul(grad_scores, query_tile)
            grad_queries.append(contract_rows(key_rows[:keys], grad_scores))
        turned = jnp.concatenate(grad_queries, axis=0).T * HD ** (-0.5)
        dq_ref[start:keys, :] = unrotate(
            turned, cosine[start:keys], sine[start:keys]
        ).astype(jnp.bfloat16)
    for own in range(groups):

        @pl.when(group == own)
        def _():
            columns = slice(own * HD, (own + 1) * HD)
            dk_ref[:, columns] = dk_sum[...] * HD ** (-0.5)
            dv_ref[:, columns] = dv_sum[...].astype(jnp.bfloat16)

    @pl.when(group == groups - 1)
    def _():
        narrow = dk_ref.shape[1]
        dk_ref[...] = unrotate(dk_ref[...], cosine[:, :narrow], sine[:, :narrow])


def attention_specs(rows, heads_width, keys_width):
    groups = keys_width // HD
    width = heads_width // groups
    grid = (rows // SEQ, groups)
    wide = pl.BlockSpec((SEQ, width), lambda s, g: (s, g))
    narrow = pl.BlockSpec((SEQ, keys_width), lambda s, g: (s, 0))
    docs = [
        pl.BlockSpec((1, 1, SEQ), lambda s, g: (s, 0, 0)),
        pl.BlockSpec((SEQ, 1), lambda s, g: (s, 0)),
    ]
    tables = [pl.BlockSpec((SEQ, width), lambda s, g: (0, 0))] * 2
    return groups, grid, wide, narrow, docs, tables


def attention_cost(rows, heads_width, matmuls):
    pairs = rows * SEQ * (heads_width // HD)
    return pl.CostEstimate(
        flops=2 * matmuls * pairs * HD, transcendentals=pairs, bytes_accessed=16 * rows * heads_width
    )


def attend(query_pre, key_pre, value_pre, doc_row, doc_col, tables):
    rows, heads_width = query_pre.shape
    keys_width = key_pre.shape[1]
    groups, grid, wide, narrow, docs, table_specs = attention_specs(rows, heads_width, keys_width)
    bf = jnp.bfloat16
    return pl.pallas_call(
        functools.partial(attend_kernel, groups),
        name="attend",
        grid=grid,
        in_specs=[wide, narrow, narrow] + docs + table_specs,
        out_specs=[wide, narrow, narrow, wide],
        out_shape=[
            jax.ShapeDtypeStruct((rows, heads_width), bf),
            jax.ShapeDtypeStruct((rows, keys_width), bf),
            jax.ShapeDtypeStruct((rows, keys_width), bf),
            jax.ShapeDtypeStruct((rows, heads_width), bf),
        ],
        cost_estimate=attention_cost(rows, heads_width, 2),
    )(query_pre, key_pre, value_pre, doc_row, doc_col, *tables)


def attend_back(query_rows, key_rows, value_rows, grad_mixed, doc_row, doc_col, tables):
    rows, heads_width = query_rows.shape
    keys_width = key_rows.shape[1]
    groups, grid, wide, narrow, docs, table_specs = attention_specs(rows, heads_width, keys_width)
    bf = jnp.bfloat16
    return pl.pallas_call(
        functools.partial(attend_back_kernel, groups),
        name="attend_back",
        grid=grid,
        in_specs=[wide, narrow, narrow, wide] + docs + table_specs,
        out_specs=[wide, narrow, narrow],
        out_shape=[
            jax.ShapeDtypeStruct((rows, heads_width), bf),
            jax.ShapeDtypeStruct((rows, keys_width), jnp.float32),
            jax.ShapeDtypeStruct((rows, keys_width), bf),
        ],
        scratch_shapes=[pltpu.VMEM((SEQ, HD), jnp.float32)] * 2,
        cost_estimate=attention_cost(rows, heads_width, 5),
    )(query_rows, key_rows, value_rows, grad_mixed, doc_row, doc_col, *tables)


def swap(array, axis, size, bit):
    return lax.ppermute(array, axis, [(i, i ^ bit) for i in range(size)])


def gather_rows(own, size):
    if size != 4:
        return lax.all_gather(own, "tensor", axis=0, tiled=True)
    me = lax.axis_index("tensor")
    rows = own.shape[0]
    half = rows // 2
    near_x = swap(own, "tensor", size, 1)
    near_y = swap(own, "tensor", size, 2)
    far_low = swap(near_x[:half], "tensor", size, 2)
    far_high = swap(near_y[half:], "tensor", size, 1)
    whole = jnp.zeros((size * rows,) + own.shape[1:], own.dtype)
    far = (me ^ 3) * rows
    for piece, at in (
        (own, me * rows),
        (near_x, (me ^ 1) * rows),
        (near_y, (me ^ 2) * rows),
        (far_low, far),
        (far_high, far + half),
    ):
        whole = lax.dynamic_update_slice_in_dim(whole, piece, at, 0)
    return whole


def sum_rows(partial, size, beside=None):
    partial = partial.astype(jnp.bfloat16)
    if size != 4:
        return lax.psum_scatter(
            partial, "tensor", scatter_dimension=0, tiled=True
        ).astype(jnp.float32)
    me = lax.axis_index("tensor")
    rows = partial.shape[0] // size
    half = rows // 2

    def part(index, start=0, count=rows):
        return lax.dynamic_slice_in_dim(partial, index * rows + start, count, 0)

    from_x = swap(part(me ^ 3, 0, half), "tensor", size, 1)
    from_y = swap(part(me ^ 3, half, half), "tensor", size, 2)
    wide = jnp.float32
    near_low, near_high = part(me ^ 2, 0, half), part(me ^ 1, half, half)
    if beside is not None:
        near_low, near_high, _ = lax.optimization_barrier((near_low, near_high, beside))
    near_low = (near_low.astype(wide) + from_x.astype(wide)).astype(jnp.bfloat16)
    near_high = (near_high.astype(wide) + from_y.astype(wide)).astype(jnp.bfloat16)
    to_y = jnp.concatenate([near_low, part(me ^ 2, half, half)])
    to_x = jnp.concatenate([part(me ^ 1, 0, half), near_high])
    last_y = swap(to_y, "tensor", size, 2)
    last_x = swap(to_x, "tensor", size, 1)
    return part(me).astype(wide) + last_x.astype(wide) + last_y.astype(wide)


def sum_all(array, axis, size):
    if size & (size - 1):
        return lax.psum(array, axis)
    bit = 1
    while bit < size:
        array = array + swap(array, axis, size, bit)
        bit *= 2
    return array


def parity_columns(rows, size):
    mine = lax.axis_index("dp") % 2
    cut = rows.reshape(rows.shape[0], size // 2, 2, rows.shape[1] // size)

    def pick(which):
        return lax.dynamic_index_in_dim(cut, which, 2, keepdims=False).reshape(rows.shape[0], -1)

    return pick(mine), pick(1 - mine)


def other_grad(parities, right_side):
    return contract_rows(parities[1], right_side).astype(jnp.bfloat16)


def pair_grad(parities, right_side, size, other=None):
    other = other_grad(parities, right_side) if other is None else other
    from_pair = swap(other, "dp", size, 1)
    pair_sum = contract_rows(parities[0], right_side) + from_pair.astype(jnp.float32)
    return pair_sum.astype(jnp.bfloat16)


def sum_pairs(pair_sum, size):
    groups = [list(range(0, size, 2)), list(range(1, size, 2))]
    return lax.psum_scatter(
        pair_sum,
        "dp",
        scatter_dimension=0,
        tiled=True,
        axis_index_groups=groups,
    ).astype(jnp.float32)


def per_device(
    dp,
    tp,
    block_input,
    attn_gain,
    w_query,
    w_key,
    w_value,
    w_out,
    mlp_gain,
    w_gate,
    w_up,
    w_down,
    doc_ids,
    cotangent,
):
    heads_width, keys_width = w_query.shape[1], w_key.shape[1]
    splits = (heads_width, heads_width + keys_width)

    def gather(weight):
        return lax.all_gather(weight, "dp", axis=0, tiled=True)

    narrow = splits[1] + keys_width
    small_full = gather(jnp.concatenate([w_query, w_key, w_value, w_out], axis=1))
    qkv_full, out_full = small_full[:, :narrow], small_full[:, narrow:]
    gate_up_full = gather(jnp.concatenate([w_gate, w_up], axis=1))
    gate_full, up_full = jnp.split(gate_up_full, 2, axis=1)
    down_full = gather(w_down)

    live_all = (doc_ids >= 0).astype(jnp.float32)
    doc_row = doc_ids.reshape(-1, 1, SEQ)
    doc_col = doc_ids.reshape(-1, 1)
    tables = rotary_tables(SEQ, HD, heads_width // keys_width)

    input_own = block_input.astype(jnp.float32)
    scale_one = norm_scale(input_own)
    normed_one = gather_rows(
        (input_own * scale_one * attn_gain[None, :]).astype(jnp.bfloat16), tp
    )
    grad_full = gather_rows(cotangent, tp)

    qkv_pre = matmul(normed_one, qkv_full)
    query_rows, key_rows, value_rows, mixed_all = attend(
        *jnp.split(qkv_pre, splits, axis=1), doc_row, doc_col, tables
    )
    residual_own = input_own + sum_rows(contract_cols(mixed_all, out_full), tp)
    scale_two_own = norm_scale(residual_own)
    normed_two = gather_rows(
        (residual_own * scale_two_own * mlp_gain[None, :]).astype(jnp.bfloat16), tp
    )
    gate_pre = matmul(normed_two, gate_full)
    up_pre = matmul(normed_two, up_full)
    sigmoid_gate = jax.nn.sigmoid(gate_pre)
    silu_gate = gate_pre * sigmoid_gate
    hidden = (silu_gate * up_pre).astype(jnp.bfloat16)
    pair_down = pair_grad(parity_columns(grad_full, dp), hidden, dp)
    one_parities = parity_columns(normed_one, dp)
    two_parities = parity_columns(normed_two, dp)
    pair_down, down_full, one_parities, two_parities = lax.optimization_barrier(
        (pair_down, down_full, one_parities, two_parities)
    )
    grad_down = sum_pairs(pair_down, dp)

    grad_hidden = matmul(grad_full, down_full)
    grad_gate_pre = (
        grad_hidden * up_pre * sigmoid_gate * (1.0 + gate_pre * (1.0 - sigmoid_gate))
    ).astype(jnp.bfloat16)
    grad_up_pre = (grad_hidden * silu_gate).astype(jnp.bfloat16)
    grad_gate_up = jnp.concatenate(
        lax.optimization_barrier((grad_gate_pre, grad_up_pre)), axis=1
    )
    other_gate_up = other_grad(two_parities, grad_gate_up)
    other_gate_up, grad_gate_up = lax.optimization_barrier((other_gate_up, grad_gate_up))
    grad_normed_part = contract_cols(grad_gate_up, gate_up_full).astype(jnp.bfloat16)
    grad_normed_part, grad_gate_up = lax.optimization_barrier((grad_normed_part, grad_gate_up))
    pair_gate_up = pair_grad(two_parities, grad_gate_up, dp, other_gate_up)
    grad_normed_own = sum_rows(grad_normed_part, tp, beside=pair_gate_up)
    grad_gate, grad_up = jnp.split(sum_pairs(pair_gate_up, dp), 2, axis=1)
    grad_mlp_gain = jnp.sum(grad_normed_own * residual_own * scale_two_own, axis=0)
    grad_residual_own = cotangent.astype(jnp.float32) + norm_back(
        grad_normed_own, residual_own, scale_two_own, mlp_gain
    )
    to_gather, hidden = lax.optimization_barrier(
        (grad_residual_own.astype(jnp.bfloat16), hidden)
    )
    grad_residual_bf = gather_rows(to_gather, tp)
    block_part = contract_cols(hidden, down_full).astype(jnp.bfloat16)
    grad_residual_bf, block_part = lax.optimization_barrier((grad_residual_bf, block_part))
    grad_mixed = (matmul(grad_residual_bf, out_full) * live_all[:, None]).astype(jnp.bfloat16)
    block_output = (residual_own + sum_rows(block_part, tp)).astype(jnp.bfloat16)
    grad_query_rows, grad_keys, grad_value_rows = attend_back(
        query_rows, key_rows, value_rows, grad_mixed, doc_row, doc_col, tables
    )
    grad_qkv_rows = jnp.concatenate(
        [grad_query_rows, grad_keys.astype(jnp.bfloat16), grad_value_rows], axis=1
    )
    grad_one_part = contract_cols(grad_qkv_rows, qkv_full).astype(jnp.bfloat16)
    grad_one_part, grad_qkv_rows, mixed_all, grad_residual_bf = lax.optimization_barrier(
        (grad_one_part, grad_qkv_rows, mixed_all, grad_residual_bf)
    )
    pair_small = jnp.concatenate(
        [
            pair_grad(one_parities, grad_qkv_rows, dp),
            pair_grad(parity_columns(grad_residual_bf, dp), mixed_all, dp),
        ],
        axis=1,
    )
    pair_small = with_layout_constraint(pair_small, Layout(major_to_minor=(0, 1)))
    grad_query, grad_key, grad_value, grad_out = jnp.split(
        sum_pairs(pair_small, dp), splits + (narrow,), axis=1
    )
    grad_normed_one = sum_rows(grad_one_part, tp)
    grad_attn_gain = jnp.sum(grad_normed_one * input_own * scale_one, axis=0)
    input_grad = (
        grad_residual_own + norm_back(grad_normed_one, input_own, scale_one, attn_gain)
    ).astype(jnp.bfloat16)
    gains = jnp.stack([grad_attn_gain, grad_mlp_gain])
    gains = sum_all(sum_all(gains, "tensor", tp), "dp", dp)
    return (
        block_output,
        input_grad,
        grad_query,
        grad_key,
        grad_value,
        grad_out,
        grad_gate,
        grad_up,
        grad_down,
        gains[0],
        gains[1],
    )


def solution(mesh):
    in_specs = (
        P(("dp", "tensor"), None),
        P(),
        P("dp", "tensor"),
        P("dp", "tensor"),
        P("dp", "tensor"),
        P("dp", "tensor"),
        P(),
        P("dp", "tensor"),
        P("dp", "tensor"),
        P("dp", "tensor"),
        P("dp"),
        P(("dp", "tensor"), None),
    )
    out_specs = (
        P(("dp", "tensor"), None),
        P(("dp", "tensor"), None),
        P("dp", "tensor"),
        P("dp", "tensor"),
        P("dp", "tensor"),
        P("dp", "tensor"),
        P("dp", "tensor"),
        P("dp", "tensor"),
        P("dp", "tensor"),
        P(),
        P(),
    )
    return jax.shard_map(
        functools.partial(per_device, mesh.shape["dp"], mesh.shape["tensor"]),
        mesh=mesh,
        in_specs=in_specs,
        out_specs=out_specs,
        check_vma=False,
    )
```
